256 devices in a mesh: section: 2 (over y_hi), pen: 64 (over y_lo, z, x), slab: 2 (over core).
Axes of the slice: x: 4, y: 4 (y_hi: 2, y_lo: 2; y = y_hi * 2 + y_lo), z: 8, core: 2. Of those that a mesh axis runs over, the one named last changes fastest.
Arguments:
- velocity: float32 [3, 384, 384, 384], P(None, ('section', 'pen'), 'slab'), may hold values from -6 to 6
- vorticity: float32 [3, 384, 384, 384], P(None, ('section', 'pen'), 'slab'), may hold values from -6 to 6
- velocity_modes: float32 [3, 256, 256, 2, 256], P(None, None, ('section', 'pen'), None, 'slab'), may hold values from -6 to 6
Outputs:
- rhs_modes: float32 [3, 256, 256, 2, 256], P(None, None, ('section', 'pen'), None, 'slab')
The draws below stay inside these ranges and needn't reach their ends.
All inputs are finite; a program needn't handle non-finite values.
Results may differ from the reference program's by a relative error of at most 0.000057.
Values sent between devices are 32-bit elements; how exact they have to be, the bound alone decides.
No kernel may reach another device: no remote copies, remote signals or barrier semaphores. Data moves between devices by JAX's collectives and lax.ppermute only.
A program may use at most 64 MiB of HBM per device.

```python
import jax
import jax.numpy as jnp
from jax import lax

N = 384
KEEP = 256


def block_levels(stream_key, shape, split, low, top_value):
    def one(position, blocks):
        steps = jax.random.uniform(jax.random.fold_in(jax.random.fold_in(stream_key, 6), position), (blocks,), jnp.float32, low / len(split), top_value / len(split))
        return jnp.repeat(jnp.exp(steps), shape[position] // blocks).reshape((-1,) + (1,) * (len(shape) - position - 1))

    loudness = one(*split[0])
    for cut in split[1:]:
        loudness = loudness * one(*cut)
    return loudness


def centred(stream_key, shape, deviation, most, split=(), kind=jnp.bfloat16):
    drawn = deviation * jax.random.normal(stream_key, shape, jnp.float32)
    if split:
        drawn = drawn * block_levels(stream_key, shape, split, -0.22, 0.18)
    return jnp.clip(drawn, -most, most).astype(kind)


def setup_inputs(seed: int = 0) -> dict:
    streams_of = jax.random.split(jax.random.key(seed), 4)
    return {
        "velocity": centred(streams_of[0], (3, N, N, N), 1.0, 6.0, ((1, 128), (2, 2)), jnp.float32),
        "vorticity": centred(streams_of[1], (3, N, N, N), 1.0, 6.0, ((1, 128), (2, 2)), jnp.float32),
        "velocity_modes": centred(streams_of[2], (3, KEEP, KEEP, 2, KEEP), 1.0, 6.0, ((2, 128), (4, 2)), jnp.float32),
    }


def signed_modes(index, count):
    return jnp.where(index < count // 2, index, index - count)


def reference(velocity, vorticity, velocity_modes):
    velocity_field = velocity
    vorticity_field = vorticity
    cross_product = jnp.stack([velocity_field[1] * vorticity_field[2] - velocity_field[2] * vorticity_field[1],
                         velocity_field[2] * vorticity_field[0] - velocity_field[0] * vorticity_field[2],
                         velocity_field[0] * vorticity_field[1] - velocity_field[1] * vorticity_field[0]])
    picked = jnp.concatenate([jnp.arange(KEEP // 2, dtype=jnp.int32),
                              jnp.arange(N - KEEP // 2, N, dtype=jnp.int32)])

    def transform(field):
        spec = jnp.fft.fft(field, axis=2, norm="ortho")[:, :, picked]
        spec = jnp.fft.fft(spec, axis=1, norm="ortho")[:, picked, :]
        spec = jnp.fft.fft(spec, axis=0, norm="ortho")[picked]
        return jnp.stack([jnp.real(spec), jnp.imag(spec)])

    spectrum = lax.map(transform, cross_product)
    modes = signed_modes(jnp.arange(KEEP, dtype=jnp.int32), KEEP)
    kz = modes[:, None, None]
    ky = modes[None, :, None]
    kx = modes[None, None, :]
    limit = -(KEEP // 2)
    mask = ((kx != limit) & (ky != limit) & (kz != limit)).astype(jnp.float32)
    waves = (kx.astype(jnp.float32), ky.astype(jnp.float32), kz.astype(jnp.float32))
    ksq = waves[0] * waves[0] + waves[1] * waves[1] + waves[2] * waves[2]
    denom = jnp.maximum(ksq, 1.0)
    parts = []
    for which in range(2):
        comp = [spectrum[c, which] for c in range(3)]
        inner = (waves[0] * comp[0] + waves[1] * comp[1] + waves[2] * comp[2]) / denom
        parts.append(jnp.stack([comp[c] - waves[c] * inner for c in range(3)]))
    projected = jnp.stack(parts, axis=3)
    visc = 0.5 / (KEEP // 2) ** 2
    return projected * mask[None, :, :, None, :] - visc * ksq[None, :, :, None, :] * velocity_modes
```

```python
import functools
import math

import jax
import jax.numpy as jnp
import ml_dtypes
import numpy as np
from jax import lax
from jax.experimental import pallas as pl
from jax.experimental.pallas import tpu as pltpu
from jax.sharding import PartitionSpec as P

VMEM = pltpu.VMEM
GROUP = ("section", "pen")


def signed(index, count):
    return np.where(index < count // 2, index, index - count)


def halves(table):
    high = table.astype(np.float32).astype(ml_dtypes.bfloat16)
    low = (table - high.astype(np.float64)).astype(np.float32).astype(ml_dtypes.bfloat16)
    return high, low


def angles(modes, positions, length):
    return 2.0 * math.pi / length * ((modes[:, None] * positions[None, :]) % length)


def x_table(cells, keep):
    modes = signed(np.arange(keep), keep)
    theta = angles(modes, np.arange(cells), cells).T / 1.0
    block = keep // 2
    parts = []
    for h in range(2):
        cut = theta[:, h * block : (h + 1) * block]
        parts += [np.cos(cut), -np.sin(cut)]
    high, low = halves(np.concatenate(parts, axis=1) / math.sqrt(cells))
    return np.concatenate([high, low, high], axis=0)


def y_table(cells, keep):
    modes = signed(np.arange(keep), keep)
    out = []
    for parity in range(2):
        theta = angles(modes[parity::2], np.arange(cells // 2), cells)
        high, low = halves(np.concatenate([np.cos(theta), np.sin(theta)], axis=0) / math.sqrt(cells))
        out.append(np.concatenate([high, high, low], axis=1))
    return np.stack(out)


def z_table(cells, keep, planes):
    modes = signed(np.arange(keep), keep)
    positions = np.arange(cells).reshape(cells // planes, planes).T.reshape(-1)
    theta = angles(modes, positions, cells)
    high, low = halves(np.concatenate([np.cos(theta), np.sin(theta)], axis=0) / math.sqrt(cells))
    return np.concatenate([high, high, low], axis=1)


def split(x):
    high = x.astype(jnp.bfloat16)
    low = (x - high.astype(jnp.float32)).astype(jnp.bfloat16)
    return high, low


def product(a, b):
    return jnp.dot(a, b, preferred_element_type=jnp.float32)


def x_kernel(plane, v_ref, w_ref, table_ref, keep_ref, send_ref):
    slab = lax.axis_index("slab")
    half = keep_ref.shape[-1]
    rows = v_ref.shape[2]
    for c in range(3):
        a, b = (c + 1) % 3, (c + 2) % 3
        cross = v_ref[a, plane] * w_ref[b, plane] - v_ref[b, plane] * w_ref[a, plane]
        high, low = split(cross)
        out = product(jnp.concatenate([high, high, low], axis=1), table_ref[...])
        first, second = out[:, :half], out[:, half:]
        mine = slab == 0
        keep_ref[c * rows : (c + 1) * rows] = jnp.where(mine, first, second)
        send_ref[c * rows : (c + 1) * rows] = jnp.where(mine, second, first)


def y_kernel(planes, *refs):
    keeps, gots = refs[:planes], refs[planes : 2 * planes]
    table_ref, out_ref = refs[2 * planes :]
    sign = jnp.where(lax.axis_index("slab") == 0, 1.0, -1.0).astype(jnp.float32)
    dests = table_ref.shape[1] // 2
    rows = keeps[0].shape[0] // 3
    lanes = keeps[0].shape[1] // 2
    per = out_ref.shape[0] // dests
    for c in range(3):
        here = slice(c * rows, (c + 1) * rows)
        for plane in range(planes):
            own, got = keeps[plane][here], gots[plane][here]
            for parity in range(2):
                folded = own + got if parity == 0 else (own - got) * sign
                high, low = split(folded)
                out = product(table_ref[parity], jnp.concatenate([high, low, high], axis=0))
                base = (c * planes + plane) * 4 + parity * 2
                out_ref[pl.ds(base, dests, per), :] = out[:dests, :lanes] + out[dests:, lanes:]
                out_ref[pl.ds(base + 1, dests, per), :] = out[:dests, lanes:] - out[dests:, :lanes]


def z_kernel(planes, keep, x_ref, modes_ref, table_ref, out_ref):
    group = lax.axis_index("section") * lax.axis_size("pen") + lax.axis_index("pen")
    slab = lax.axis_index("slab")
    lanes = x_ref.shape[1]
    per = 3 * planes * 4
    sources = x_ref.shape[0] // per
    limit = -(keep // 2)
    visc = 0.5 / (keep // 2) ** 2
    row = lax.broadcasted_iota(jnp.int32, (keep, lanes), 0)
    col = lax.broadcasted_iota(jnp.int32, (keep, lanes), 1) + slab * lanes
    kz = jnp.where(row < keep // 2, row, row - keep)
    kx = jnp.where(col < keep // 2, col, col - keep)
    for parity in range(2):
        index = group * 2 + parity
        ky = jnp.where(index < keep // 2, index, index - keep)
        mask = ((kx != limit) & (kz != limit) & (ky != limit)).astype(jnp.float32)
        fx, fz = kx.astype(jnp.float32), kz.astype(jnp.float32)
        fy = ky.astype(jnp.float32)
        ksq = fx * fx + fy * fy + fz * fz
        inverse = 1.0 / jnp.maximum(ksq, 1.0)
        damp = visc * ksq
        real, imag = [], []
        for c in range(3):
            columns = []
            for q in range(2):
                base = c * planes * 4 + parity * 2 + q
                columns.append(
                    jnp.concatenate(
                        [x_ref[pl.ds(base + p * 4, sources, per), :] for p in range(planes)], axis=0
                    )
                )
            high, low = split(jnp.concatenate(columns, axis=1))
            out = product(table_ref[...], jnp.concatenate([high, low, high], axis=0))
            real.append(out[:keep, :lanes] + out[keep:, lanes:])
            imag.append(out[:keep, lanes:] - out[keep:, :lanes])
        for q, s in enumerate((real, imag)):
            inner = (fx * s[0] + fy * s[1] + fz * s[2]) * inverse
            for c, k in enumerate((fx, fy, fz)):
                where = pl.ds(c * keep * 4 + parity * 2 + q, keep, 4)
                out_ref[where, :] = mask * (s[c] - k * inner) - damp * modes_ref[where, :]


def call(kernel, outs, name, flops):
    def run(*args):
        size = sum(a.size * a.dtype.itemsize for a in args) + sum(4 * math.prod(o) for o in outs)
        shapes = [jax.ShapeDtypeStruct(o, jnp.float32) for o in outs]
        return pl.pallas_call(
            kernel,
            out_shape=shapes if len(outs) > 1 else shapes[0],
            in_specs=[pl.BlockSpec(memory_space=VMEM)] * len(args),
            out_specs=[pl.BlockSpec(memory_space=VMEM)] * len(outs)
            if len(outs) > 1
            else pl.BlockSpec(memory_space=VMEM),
            name=name,
            cost_estimate=pl.CostEstimate(flops=flops, bytes_accessed=size, transcendentals=0),
            compiler_params=pltpu.CompilerParams(vmem_limit_bytes=40 << 20),
        )(*args)

    return run


def per_device(velocity, vorticity, velocity_modes):
    _, planes, rows_y, cells = velocity.shape
    _, keep, rows_ky, _, lanes = velocity_modes.shape
    dests = lax.axis_size(GROUP)
    table_x = jnp.asarray(x_table(cells, keep))
    table_y = jnp.asarray(y_table(cells, keep))
    table_z = jnp.asarray(z_table(cells, keep, planes))
    keeps, gots = [], []
    for p in range(planes):
        mine, other = call(
            functools.partial(x_kernel, p), [(3 * rows_y, keep)] * 2, f"x{p}", 2 * 9 * rows_y * cells * 2 * keep
        )(velocity, vorticity, table_x)
        keeps.append(mine)
        gots.append(lax.ppermute(other, "slab", [(0, 1), (1, 0)]))
    per = 3 * planes * 4
    packed = call(
        functools.partial(y_kernel, planes), [(dests * per, lanes)], "y", 2 * 3 * planes * 2 * keep * 3 * rows_y * keep
    )(*keeps, *gots, table_y)
    packed = packed.reshape(dests, 3 * planes, 4, lanes)
    arrived = lax.all_to_all(packed, GROUP, split_axis=0, concat_axis=0, tiled=True)
    out = call(
        functools.partial(z_kernel, planes, keep), [(3 * keep * 4, lanes)], "z", 2 * 6 * 2 * keep * 3 * cells * keep
    )(arrived.reshape(dests * per, lanes), velocity_modes.reshape(3 * keep * 4, lanes), table_z)
    return out.reshape(3, keep, rows_ky, 2, lanes)


def solution(mesh):
    return jax.shard_map(
        per_device,
        mesh=mesh,
        in_specs=(
            P(None, GROUP, "slab", None),
            P(None, GROUP, "slab", None),
            P(None, None, GROUP, None, "slab"),
        ),
        out_specs=P(None, None, GROUP, None, "slab"),
        check_vma=False,
    )
```

```python
import functools
import math

import jax
import jax.numpy as jnp
import ml_dtypes
import numpy as np
from jax import lax
from jax.experimental import pallas as pl
from jax.experimental.pallas import tpu as pltpu
from jax.sharding import PartitionSpec as P

VMEM = pltpu.VMEM
GROUP = ("section", "pen")
NY, NZ, NX = 4, 8, 4
NXY = NX * NY


def signed(index, count):
    return np.where(index < count // 2, index, index - count)


def halves(table):
    high = table.astype(np.float32).astype(ml_dtypes.bfloat16)
    low = (table - high.astype(np.float64)).astype(np.float32).astype(ml_dtypes.bfloat16)
    return high, low


def angles(modes, positions, length):
    return 2.0 * math.pi / length * ((modes[:, None] * positions[None, :]) % length)


def rows_of(theta, cells):
    return np.stack(halves(np.concatenate([np.cos(theta), np.sin(theta)], axis=0) / math.sqrt(cells)))


def z_major_groups():
    return np.array([(y * NZ + z) * NX + x for z in range(NZ) for y in range(NY) for x in range(NX)])


def xy_major_groups():
    return np.array([(y * NZ + z) * NX + x for y in range(NY) for x in range(NX) for z in range(NZ)])


def x_table(cells, keep):
    theta = angles(signed(np.arange(keep), keep), np.arange(cells), cells).T
    block = keep // 2
    parts = []
    for h in range(2):
        cut = theta[:, h * block : (h + 1) * block]
        parts += [np.cos(cut), -np.sin(cut)]
    return np.concatenate(halves(np.concatenate(parts, axis=1) / math.sqrt(cells)), axis=0)


def y_table(cells, keep, order):
    modes = signed(np.arange(keep), keep)
    return np.stack(
        [rows_of(angles(modes[parity::2][order], np.arange(cells // 2), cells), cells) for parity in range(2)]
    )


def z_table(cells, keep, positions):
    return rows_of(angles(signed(np.arange(keep), keep), positions, cells), cells)


def split(x):
    high = x.astype(jnp.bfloat16)
    low = (x - high.astype(jnp.float32)).astype(jnp.bfloat16)
    return high, low


def product(a, b):
    return jnp.dot(a, b, preferred_element_type=jnp.float32)


def transformed(high_table, low_table, x):
    high, low = split(x)
    return product(
        jnp.concatenate([high_table, high_table, low_table], axis=1), jnp.concatenate([high, low, high], axis=0)
    )


def place():
    pen = lax.axis_index("pen")
    x = lax.rem(pen, NX)
    z = lax.rem(lax.div(pen, NX), NZ)
    y = lax.axis_index("section") * 2 + lax.div(pen, NX * NZ)
    return y, z, x


def x_kernel(planes, v_hbm, w_hbm, table_hbm, _, keep_ref, send_ref, v_ref, w_ref, table_ref, sems):
    rows = v_ref.shape[2]
    half = keep_ref.shape[-1]
    copies = []
    for i, plane in enumerate(planes):
        for c in range(3):
            copies.append(pltpu.make_async_copy(v_hbm.at[c, plane], v_ref.at[i, c], sems.at[i * 6 + c]))
            copies.append(pltpu.make_async_copy(w_hbm.at[c, plane], w_ref.at[i, c], sems.at[i * 6 + 3 + c]))
        if i == 0:
            copies.append(pltpu.make_async_copy(table_hbm, table_ref, sems.at[len(planes) * 6]))
    for copy in copies:
        copy.start()
    mine = lax.axis_index("slab") == 0
    deep = table_ref.shape[0] // 2
    for i in range(len(planes)):
        for copy in copies[:7] if i == 0 else copies[7 + (i - 1) * 6 : 7 + i * 6]:
            copy.wait()
        table = jnp.concatenate([table_ref[:deep], table_ref[:deep], table_ref[deep:]], axis=0)
        for c in range(3):
            a, b = (c + 1) % 3, (c + 2) % 3
            high, low = split(v_ref[i, a] * w_ref[i, b] - v_ref[i, b] * w_ref[i, a])
            out = product(jnp.concatenate([high, low, high], axis=1), table)
            first, second = out[:, :half], out[:, half:]
            here = slice((i * 3 + c) * rows, (i * 3 + c + 1) * rows)
            keep_ref[here] = jnp.where(mine, first, second)
            send_ref[here] = jnp.where(mine, second, first)


def y_blocks(keep_ref, got_ref, table_ref, rows):
    sign = jnp.where(lax.axis_index("slab") == 0, 1.0, -1.0).astype(jnp.float32)
    dests = table_ref.shape[2] // 2
    lanes = keep_ref.shape[1] // 2
    for block in range(keep_ref.shape[0] // rows):
        here = slice(block * rows, (block + 1) * rows)
        own, got = keep_ref[here], got_ref[here]
        for parity in range(2):
            folded = own + got if parity == 0 else (own - got) * sign
            out = transformed(table_ref[parity, 0], table_ref[parity, 1], folded)
            yield block, parity * 2, out[:dests, :lanes] + out[dests:, lanes:]
            yield block, parity * 2 + 1, out[:dests, lanes:] - out[dests:, :lanes]


def y_pack_kernel(rows, keep_ref, got_ref, table_ref, _, out_ref):
    dests = table_ref.shape[2] // 2
    per = out_ref.shape[0] // dests
    for block, q, value in y_blocks(keep_ref, got_ref, table_ref, rows):
        out_ref[pl.ds(block * 4 + q, dests, per), :] = value


def y_send_kernel(rows, keep_ref, got_ref, table_ref, *refs):
    outs, all_ref = refs[:-1], refs[-1]
    dests = table_ref.shape[2] // 2
    for block, q, value in y_blocks(keep_ref, got_ref, table_ref, rows):
        at = (block * 4 + q) * dests
        all_ref[at : at + dests] = value
    _, z, _ = place()
    for shift in range(NZ):
        to = lax.rem(z - shift + NZ, NZ)
        for k in range(all_ref.shape[0] // dests):
            outs[shift][k * NXY : (k + 1) * NXY] = all_ref[pl.ds(pl.multiple_of(k * dests + to * NXY, NXY), NXY), :]


def turn_kernel(*refs):
    gots, outs, all_ref = refs[:NZ], refs[NZ:-1], refs[-1]
    y, z, x = place()
    size = gots[0].shape[0]
    for shift in range(NZ):
        source = lax.rem(z + shift, NZ)
        all_ref[pl.ds(pl.multiple_of(source * size, size), size), :] = gots[shift][...]
    count = all_ref.shape[0] // NXY
    for dy in range(NY):
        for dx in range(NX):
            to = lax.rem(y - dy + NY, NY) * NX + lax.rem(x - dx + NX, NX)
            outs[dy * NX + dx][...] = all_ref[pl.ds(to, count, NXY), :]


def early_kernel(keep, *refs):
    gots, table_ref, out_ref, all_ref = refs[:NXY], refs[NXY], refs[NXY + 1], refs[NXY + 2]
    y, _, x = place()
    lanes = out_ref.shape[1]
    kinds = gots[0].shape[0] // NZ
    sources = NXY * NZ
    for dy in range(NY):
        for dx in range(NX):
            source = lax.rem(y + dy, NY) * NX + lax.rem(x + dx, NX)
            for k in range(kinds):
                at = pl.multiple_of(k * sources + source * NZ, NZ)
                all_ref[pl.ds(at, NZ), :] = gots[dy * NX + dx][pl.ds(k, NZ, kinds), :]
    for pair in range(kinds // 2):
        both = [all_ref[(pair * 2 + q) * sources : (pair * 2 + q + 1) * sources] for q in range(2)]
        out = transformed(table_ref[0], table_ref[1], jnp.concatenate(both, axis=1))
        out_ref[pair * 2 * keep : (pair * 2 + 1) * keep] = out[:keep, :lanes] + out[keep:, lanes:]
        out_ref[(pair * 2 + 1) * keep : (pair * 2 + 2) * keep] = out[:keep, lanes:] - out[keep:, :lanes]


def z_kernel(planes, keep, x_ref, early_ref, modes_ref, table_ref, out_ref):
    group = lax.axis_index("section") * lax.axis_size("pen") + lax.axis_index("pen")
    slab = lax.axis_index("slab")
    lanes = x_ref.shape[1]
    per = 3 * planes * 4
    sources = x_ref.shape[0] // per
    limit = -(keep // 2)
    visc = 0.5 / (keep // 2) ** 2
    row = lax.broadcasted_iota(jnp.int32, (keep, lanes), 0)
    col = lax.broadcasted_iota(jnp.int32, (keep, lanes), 1) + slab * lanes
    kz = jnp.where(row < keep // 2, row, row - keep)
    kx = jnp.where(col < keep // 2, col, col - keep)
    for parity in range(2):
        index = group * 2 + parity
        ky = jnp.where(index < keep // 2, index, index - keep)
        mask = ((kx != limit) & (kz != limit) & (ky != limit)).astype(jnp.float32)
        fx, fz = kx.astype(jnp.float32), kz.astype(jnp.float32)
        fy = ky.astype(jnp.float32)
        ksq = fx * fx + fy * fy + fz * fz
        inverse = 1.0 / jnp.maximum(ksq, 1.0)
        damp = visc * ksq
        real, imag = [], []
        for c in range(3):
            columns = []
            for q in range(2):
                base = parity * 2 + q
                columns.append(
                    jnp.concatenate(
                        [x_ref[pl.ds(base + (p * 3 + c) * 4, sources, per), :] for p in range(planes)], axis=0
                    )
                )
            out = transformed(table_ref[0], table_ref[1], jnp.concatenate(columns, axis=1))
            at = (c * 2 + parity) * 2 * keep
            real.append(early_ref[at : at + keep] + (out[:keep, :lanes] + out[keep:, lanes:]))
            imag.append(early_ref[at + keep : at + 2 * keep] + (out[:keep, lanes:] - out[keep:, :lanes]))
        for q, s in enumerate((real, imag)):
            inner = (fx * s[0] + fy * s[1] + fz * s[2]) * inverse
            for c, k in enumerate((fx, fy, fz)):
                where = pl.ds(c * keep * 4 + parity * 2 + q, keep, 4)
                out_ref[where, :] = mask * (s[c] - k * inner) - damp * modes_ref[where, :]


def call(kernel, outs, flops=0, scratch=(), spaces=None, limit=40 << 20):
    def run(*args):
        size = sum(a.size * a.dtype.itemsize for a in args) + sum(4 * math.prod(o) for o in outs)
        shapes = [jax.ShapeDtypeStruct(o, jnp.float32) for o in outs]
        specs = [pl.BlockSpec(memory_space=VMEM)] * len(outs)
        single = len(outs) == 1
        return pl.pallas_call(
            kernel,
            out_shape=shapes[0] if single else shapes,
            in_specs=[pl.BlockSpec(memory_space=s) for s in spaces or [VMEM] * len(args)],
            out_specs=specs[0] if single else specs,
            scratch_shapes=list(scratch),
            cost_estimate=pl.CostEstimate(flops=flops, bytes_accessed=size, transcendentals=0),
            compiler_params=pltpu.CompilerParams(vmem_limit_bytes=limit),
        )(*args)

    return run


def group_of(y, z, x):
    return ((y % NY) * NZ + z % NZ) * NX + x % NX


def from_shift(value, dy, dz, dx):
    pairs = [
        (group_of(y + dy, z + dz, x + dx), group_of(y, z, x))
        for y in range(NY)
        for z in range(NZ)
        for x in range(NX)
    ]
    return lax.ppermute(value, GROUP, pairs)


def per_device(velocity, vorticity, velocity_modes):
    _, planes, rows_y, cells = velocity.shape
    _, keep, rows_ky, _, lanes = velocity_modes.shape
    dests = lax.axis_size(GROUP)
    order = z_major_groups()
    table_y = jnp.asarray(y_table(cells, keep, order))
    table_x = jnp.asarray(x_table(cells, keep))
    keeps, gots = [], []
    for held in ([0], list(range(1, planes))):
        n = len(held)
        run = call(
            functools.partial(x_kernel, held),
            [(3 * n * rows_y, keep)] * 2,
            2 * 9 * n * rows_y * cells * 2 * keep,
            [
                VMEM((n, 3, rows_y, cells), jnp.float32),
                VMEM((n, 3, rows_y, cells), jnp.float32),
                VMEM(table_x.shape, jnp.bfloat16),
                pltpu.SemaphoreType.DMA((6 * n + 1,)),
            ],
            [pltpu.HBM] * 4,
            50 << 20,
        )
        mine, other = run(velocity, vorticity, table_x, keeps[0] if keeps else vorticity)
        keeps.append(mine)
        gots.append(lax.ppermute(other, "slab", [(0, 1), (1, 0)]))
    flops = 2 * 3 * 2 * keep * 3 * rows_y * keep
    kinds = 3 * 4
    sent = call(
        functools.partial(y_send_kernel, rows_y),
        [(kinds * NXY, lanes)] * NZ,
        flops,
        [VMEM((kinds * dests, lanes), jnp.float32)],
    )(keeps[0], gots[0], table_y)
    arrived = [sent[0]]
    for s in range(1, NZ):
        arrived.append(from_shift(sent[s], 0, s, 0))
    per = (planes - 1) * kinds
    packed = call(
        functools.partial(y_pack_kernel, rows_y),
        [(dests * per, lanes)],
        flops * (planes - 1),
        spaces=[VMEM] * 3 + [pl.ANY],
    )(keeps[1], gots[1], table_y, sent[0])
    late = lax.all_to_all(
        packed.reshape(dests, per, lanes), GROUP, 0, 0, axis_index_groups=[order.tolist()], tiled=True
    )
    turned = call(turn_kernel, [(NZ * kinds, lanes)] * NXY, 0, [VMEM((NZ * kinds * NXY, lanes), jnp.float32)])(*arrived)
    spread = [turned[0]] + [from_shift(turned[d], d // NX, 0, d % NX) for d in range(1, NXY)]
    early = call(
        functools.partial(early_kernel, keep),
        [(kinds * keep, lanes)],
        2 * 6 * 2 * keep * 3 * dests * keep,
        [VMEM((kinds * dests, lanes), jnp.float32)],
    )(*spread, jnp.asarray(z_table(cells, keep, planes * xy_major_groups())))
    rest = np.concatenate([planes * order + p for p in range(1, planes)])
    out = call(
        functools.partial(z_kernel, planes - 1, keep),
        [(3 * keep * 4, lanes)],
        2 * 6 * 2 * keep * 3 * (planes - 1) * dests * keep,
    )(
        late.reshape(dests * per, lanes),
        early,
        velocity_modes.reshape(3 * keep * 4, lanes),
        jnp.asarray(z_table(cells, keep, rest)),
    )
    return out.reshape(3, keep, rows_ky, 2, lanes)


def solution(mesh):
    return jax.shard_map(
        per_device,
        mesh=mesh,
        in_specs=(
            P(None, GROUP, "slab", None),
            P(None, GROUP, "slab", None),
            P(None, None, GROUP, None, "slab"),
        ),
        out_specs=P(None, None, GROUP, None, "slab"),
        check_vma=False,
    )
```

```python
import functools
import math

import jax
import jax.numpy as jnp
import ml_dtypes
import numpy as np
from jax import lax
from jax.experimental import pallas as pl
from jax.experimental.pallas import tpu as pltpu
from jax.sharding import PartitionSpec as P

VMEM = pltpu.VMEM
GROUP = ("section", "pen")
NY, NZ, NX = 4, 8, 4
NXY = NX * NY


def signed(index, count):
    return np.where(index < count // 2, index, index - count)


def halves(table):
    high = table.astype(np.float32).astype(ml_dtypes.bfloat16)
    low = (table - high.astype(np.float64)).astype(np.float32).astype(ml_dtypes.bfloat16)
    return high, low


def angles(modes, positions, length):
    return 2.0 * math.pi / length * ((modes[:, None] * positions[None, :]) % length)


def rows_of(theta, cells):
    return np.stack(halves(np.concatenate([np.cos(theta), np.sin(theta)], axis=0) / math.sqrt(cells)))


def z_major_groups():
    return np.array([(y * NZ + z) * NX + x for z in range(NZ) for y in range(NY) for x in range(NX)])


def xy_major_groups():
    return np.array([(y * NZ + z) * NX + x for y in range(NY) for x in range(NX) for z in range(NZ)])


def x_table(cells, keep):
    theta = angles(signed(np.arange(keep), keep), np.arange(cells), cells).T
    block = keep // 2
    parts = []
    for h in range(2):
        cut = theta[:, h * block : (h + 1) * block]
        parts += [np.cos(cut), -np.sin(cut)]
    return np.concatenate(halves(np.concatenate(parts, axis=1) / math.sqrt(cells)), axis=0)


def y_table(cells, keep, order):
    modes = signed(np.arange(keep), keep)
    return np.stack(
        [rows_of(angles(modes[parity::2][order], np.arange(cells // 2), cells), cells) for parity in range(2)]
    )


def z_table(cells, keep, positions):
    return rows_of(angles(signed(np.arange(keep), keep), positions, cells), cells)


def split(x):
    high = x.astype(jnp.bfloat16)
    low = (x - high.astype(jnp.float32)).astype(jnp.bfloat16)
    return high, low


def product(a, b):
    return jnp.dot(a, b, preferred_element_type=jnp.float32)


def transformed(high_table, low_table, x):
    high, low = split(x)
    return product(
        jnp.concatenate([high_table, high_table, low_table], axis=1), jnp.concatenate([high, low, high], axis=0)
    )


def place():
    pen = lax.axis_index("pen")
    x = lax.rem(pen, NX)
    z = lax.rem(lax.div(pen, NX), NZ)
    y = lax.axis_index("section") * 2 + lax.div(pen, NX * NZ)
    return y, z, x


def x_kernel(planes, v_hbm, w_hbm, table_hbm, _, keep_ref, send_ref, v_ref, w_ref, table_ref, sems):
    rows = v_ref.shape[2]
    half = keep_ref.shape[-1]
    copies = []
    for i, plane in enumerate(planes):
        for c in range(3):
            copies.append(pltpu.make_async_copy(v_hbm.at[c, plane], v_ref.at[i, c], sems.at[i * 6 + c]))
            copies.append(pltpu.make_async_copy(w_hbm.at[c, plane], w_ref.at[i, c], sems.at[i * 6 + 3 + c]))
        if i == 0:
            copies.append(pltpu.make_async_copy(table_hbm, table_ref, sems.at[len(planes) * 6]))
    for copy in copies:
        copy.start()
    mine = lax.axis_index("slab") == 0
    deep = table_ref.shape[0] // 2
    for i in range(len(planes)):
        for copy in copies[:7] if i == 0 else copies[7 + (i - 1) * 6 : 7 + i * 6]:
            copy.wait()
        table = jnp.concatenate([table_ref[:deep], table_ref[:deep], table_ref[deep:]], axis=0)
        for c in range(3):
            a, b = (c + 1) % 3, (c + 2) % 3
            high, low = split(v_ref[i, a] * w_ref[i, b] - v_ref[i, b] * w_ref[i, a])
            out = product(jnp.concatenate([high, low, high], axis=1), table)
            first, second = out[:, :half], out[:, half:]
            here = slice((i * 3 + c) * rows, (i * 3 + c + 1) * rows)
            keep_ref[here] = jnp.where(mine, first, second)
            send_ref[here] = jnp.where(mine, second, first)


def y_blocks(keep_ref, got_ref, table_ref, rows):
    sign = jnp.where(lax.axis_index("slab") == 0, 1.0, -1.0).astype(jnp.float32)
    dests = table_ref.shape[2] // 2
    lanes = keep_ref.shape[1] // 2
    for block in range(keep_ref.shape[0] // rows):
        here = slice(block * rows, (block + 1) * rows)
        own, got = keep_ref[here], got_ref[here]
        for parity in range(2):
            folded = own + got if parity == 0 else (own - got) * sign
            out = transformed(table_ref[parity, 0], table_ref[parity, 1], folded)
            yield block, parity * 2, out[:dests, :lanes] + out[dests:, lanes:]
            yield block, parity * 2 + 1, out[:dests, lanes:] - out[dests:, :lanes]


def y_pack_kernel(rows, keep_ref, got_ref, table_ref, _, out_ref):
    dests = table_ref.shape[2] // 2
    per = out_ref.shape[0] // dests
    for block, q, value in y_blocks(keep_ref, got_ref, table_ref, rows):
        out_ref[pl.ds(block * 4 + q, dests, per), :] = value


def y_send_kernel(rows, keep_ref, got_ref, table_ref, *refs):
    outs, all_ref = refs[:-1], refs[-1]
    dests = table_ref.shape[2] // 2
    for block, q, value in y_blocks(keep_ref, got_ref, table_ref, rows):
        at = (block * 4 + q) * dests
        all_ref[at : at + dests] = value
    _, z, _ = place()
    for shift in range(NZ):
        to = lax.rem(z - shift + NZ, NZ)
        for k in range(all_ref.shape[0] // dests):
            outs[shift][k * NXY : (k + 1) * NXY] = all_ref[pl.ds(pl.multiple_of(k * dests + to * NXY, NXY), NXY), :]


def turn_x_kernel(*refs):
    gots, outs, all_ref = refs[:NZ], refs[NZ:-1], refs[-1]
    _, z, x = place()
    size = gots[0].shape[0]
    for shift in range(NZ):
        source = lax.rem(z + shift, NZ)
        all_ref[pl.ds(pl.multiple_of(source * size, size), size), :] = gots[shift][...]
    for shift in range(NX):
        to = lax.rem(x - shift + NX, NX)
        outs[shift][...] = all_ref[pl.ds(to, all_ref.shape[0] // NX, NX), :]


def turn_y_kernel(*refs):
    gots, outs = refs[:NX], refs[NX:]
    y, _, x = place()
    size = gots[0].shape[0] // NY
    for dx in range(NX):
        at = pl.multiple_of(lax.rem(x + dx, NX) * size, size)
        for dy in range(NY):
            to = lax.rem(y - dy + NY, NY)
            outs[dy][pl.ds(at, size), :] = gots[dx][pl.ds(to, size, NY), :]


def wave_numbers(keep, lanes):
    group = lax.axis_index("section") * lax.axis_size("pen") + lax.axis_index("pen")
    limit = -(keep // 2)
    visc = 0.5 / (keep // 2) ** 2
    row = lax.broadcasted_iota(jnp.int32, (keep, lanes), 0)
    col = lax.broadcasted_iota(jnp.int32, (keep, lanes), 1) + lax.axis_index("slab") * lanes
    kz = jnp.where(row < keep // 2, row, row - keep)
    kx = jnp.where(col < keep // 2, col, col - keep)
    for parity in range(2):
        index = group * 2 + parity
        ky = jnp.where(index < keep // 2, index, index - keep)
        mask = ((kx != limit) & (kz != limit) & (ky != limit)).astype(jnp.float32)
        waves = (kx.astype(jnp.float32), ky.astype(jnp.float32), kz.astype(jnp.float32))
        ksq = waves[0] * waves[0] + waves[1] * waves[1] + waves[2] * waves[2]
        yield parity, waves, mask, 1.0 / jnp.maximum(ksq, 1.0), visc * ksq


def projected(s, waves, mask, inverse):
    inner = (waves[0] * s[0] + waves[1] * s[1] + waves[2] * s[2]) * inverse
    return [mask * (s[c] - waves[c] * inner) for c in range(3)]


def z_sums(keep, lanes, table, columns):
    out = transformed(table[0], table[1], columns)
    return out[:keep, :lanes] + out[keep:, lanes:], out[:keep, lanes:] - out[keep:, :lanes]


def early_kernel(keep, *refs):
    gots, (modes_ref, table_ref, out_ref, all_ref) = refs[:NY], refs[NY:]
    y, _, _ = place()
    lanes = out_ref.shape[1]
    kinds = gots[0].shape[0] // (NX * NZ)
    sources = NY * NX * NZ
    for dy in range(NY):
        source = lax.rem(y + dy, NY) * (NX * NZ)
        for k in range(kinds):
            at = pl.multiple_of(k * sources + source, NX * NZ)
            all_ref[pl.ds(at, NX * NZ), :] = gots[dy][pl.ds(k, NX * NZ, kinds), :]
    for parity, waves, mask, inverse, damp in wave_numbers(keep, lanes):
        sums = []
        for c in range(3):
            base = c * 4 + parity * 2
            both = [all_ref[(base + q) * sources : (base + q + 1) * sources] for q in range(2)]
            sums.append(z_sums(keep, lanes, table_ref, jnp.concatenate(both, axis=1)))
        for q in range(2):
            for c, value in enumerate(projected([s[q] for s in sums], waves, mask, inverse)):
                where = pl.ds(c * keep * 4 + parity * 2 + q, keep, 4)
                out_ref[where, :] = value - damp * modes_ref[where, :]


def z_kernel(planes, keep, x_ref, early_ref, table_hbm, out_ref, table_ref, sem):
    copy = pltpu.make_async_copy(table_hbm, table_ref, sem)
    copy.start()
    lanes = x_ref.shape[1]
    per = 3 * planes * 4
    sources = x_ref.shape[0] // per
    copy.wait()
    for parity, waves, mask, inverse, _ in wave_numbers(keep, lanes):
        sums = []
        for c in range(3):
            columns = [
                jnp.concatenate(
                    [x_ref[pl.ds((p * 3 + c) * 4 + parity * 2 + q, sources, per), :] for p in range(planes)], axis=0
                )
                for q in range(2)
            ]
            sums.append(z_sums(keep, lanes, table_ref, jnp.concatenate(columns, axis=1)))
        for q in range(2):
            for c, value in enumerate(projected([s[q] for s in sums], waves, mask, inverse)):
                where = pl.ds(c * keep * 4 + parity * 2 + q, keep, 4)
                out_ref[where, :] = value + early_ref[where, :]


def call(kernel, outs, flops=0, scratch=(), spaces=None, limit=40 << 20):
    def run(*args):
        size = sum(a.size * a.dtype.itemsize for a in args) + sum(4 * math.prod(o) for o in outs)
        shapes = [jax.ShapeDtypeStruct(o, jnp.float32) for o in outs]
        specs = [pl.BlockSpec(memory_space=VMEM)] * len(outs)
        single = len(outs) == 1
        return pl.pallas_call(
            kernel,
            out_shape=shapes[0] if single else shapes,
            in_specs=[pl.BlockSpec(memory_space=s) for s in spaces or [VMEM] * len(args)],
            out_specs=specs[0] if single else specs,
            scratch_shapes=list(scratch),
            cost_estimate=pl.CostEstimate(flops=flops, bytes_accessed=size, transcendentals=0),
            compiler_params=pltpu.CompilerParams(vmem_limit_bytes=limit),
        )(*args)

    return run


def group_of(y, z, x):
    return ((y % NY) * NZ + z % NZ) * NX + x % NX


def from_shift(value, dy, dz, dx):
    pairs = [
        (group_of(y + dy, z + dz, x + dx), group_of(y, z, x))
        for y in range(NY)
        for z in range(NZ)
        for x in range(NX)
    ]
    return lax.ppermute(value, GROUP, pairs)


def per_device(velocity, vorticity, velocity_modes):
    _, planes, rows_y, cells = velocity.shape
    _, keep, rows_ky, _, lanes = velocity_modes.shape
    dests = lax.axis_size(GROUP)
    order = z_major_groups()
    table_y = jnp.asarray(y_table(cells, keep, order))
    table_x = jnp.asarray(x_table(cells, keep))
    keeps, gots = [], []
    for held in ([0], list(range(1, planes))):
        n = len(held)
        run = call(
            functools.partial(x_kernel, held),
            [(3 * n * rows_y, keep)] * 2,
            2 * 9 * n * rows_y * cells * 2 * keep,
            [
                VMEM((n, 3, rows_y, cells), jnp.float32),
                VMEM((n, 3, rows_y, cells), jnp.float32),
                VMEM(table_x.shape, jnp.bfloat16),
                pltpu.SemaphoreType.DMA((6 * n + 1,)),
            ],
            [pltpu.HBM] * 4,
            50 << 20,
        )
        mine, other = run(velocity, vorticity, table_x, keeps[0] if keeps else vorticity)
        keeps.append(mine)
        gots.append(lax.ppermute(other, "slab", [(0, 1), (1, 0)]))
    flops = 2 * 3 * 2 * keep * 3 * rows_y * keep
    kinds = 3 * 4
    sent = call(
        functools.partial(y_send_kernel, rows_y),
        [(kinds * NXY, lanes)] * NZ,
        flops,
        [VMEM((kinds * dests, lanes), jnp.float32)],
    )(keeps[0], gots[0], table_y)
    arrived = [sent[0]]
    for s in range(1, NZ):
        arrived.append(from_shift(sent[s], 0, s, 0))
    per = (planes - 1) * kinds
    packed = call(
        functools.partial(y_pack_kernel, rows_y),
        [(dests * per, lanes)],
        flops * (planes - 1),
        spaces=[VMEM] * 3 + [pl.ANY],
    )(keeps[1], gots[1], table_y, sent[0])
    late = lax.all_to_all(
        packed.reshape(dests, per, lanes), GROUP, 0, 0, axis_index_groups=[order.tolist()], tiled=True
    )
    turned = call(
        turn_x_kernel, [(NZ * kinds * NY, lanes)] * NX, 0, [VMEM((NZ * kinds * NXY, lanes), jnp.float32)]
    )(*arrived)
    turned = [turned[0]] + [from_shift(turned[d], 0, 0, d) for d in range(1, NX)]
    turned = call(turn_y_kernel, [(NX * NZ * kinds, lanes)] * NY)(*turned)
    spread = [turned[0]] + [from_shift(turned[d], d, 0, 0) for d in range(1, NY)]
    early = call(
        functools.partial(early_kernel, keep),
        [(3 * keep * 4, lanes)],
        2 * 6 * 2 * keep * 3 * dests * keep,
        [VMEM((kinds * dests, lanes), jnp.float32)],
    )(
        *spread,
        velocity_modes.reshape(3 * keep * 4, lanes),
        jnp.asarray(z_table(cells, keep, planes * xy_major_groups())),
    )
    rest = np.concatenate([planes * order + p for p in range(1, planes)])
    table_z = jnp.asarray(z_table(cells, keep, rest))
    out = call(
        functools.partial(z_kernel, planes - 1, keep),
        [(3 * keep * 4, lanes)],
        2 * 6 * 2 * keep * 3 * (planes - 1) * dests * keep,
        [VMEM(table_z.shape, jnp.bfloat16), pltpu.SemaphoreType.DMA],
        [VMEM, VMEM, pltpu.HBM],
        40 << 20,
    )(late.reshape(dests * per, lanes), early, table_z)
    return out.reshape(3, keep, rows_ky, 2, lanes)


def solution(mesh):
    return jax.shard_map(
        per_device,
        mesh=mesh,
        in_specs=(
            P(None, GROUP, "slab", None),
            P(None, GROUP, "slab", None),
            P(None, None, GROUP, None, "slab"),
        ),
        out_specs=P(None, None, GROUP, None, "slab"),
        check_vma=False,
    )
```

```python
import functools
import math

import jax
import jax.numpy as jnp
import ml_dtypes
import numpy as np
from jax import lax
from jax.experimental import pallas as pl
from jax.experimental.pallas import tpu as pltpu
from jax.sharding import PartitionSpec as P

VMEM = pltpu.VMEM
GROUP = ("section", "pen")
NY, NZ, NX = 4, 8, 4
NXY = NX * NY


def signed(index, count):
    return np.where(index < count // 2, index, index - count)


def halves(table):
    high = table.astype(np.float32).astype(ml_dtypes.bfloat16)
    low = (table - high.astype(np.float64)).astype(np.float32).astype(ml_dtypes.bfloat16)
    return high, low


def angles(modes, positions, length):
    return 2.0 * math.pi / length * ((modes[:, None] * positions[None, :]) % length)


def rows_of(theta, cells):
    return np.stack(halves(np.concatenate([np.cos(theta), np.sin(theta)], axis=0) / math.sqrt(cells)))


def z_major_groups():
    return np.array([(y * NZ + z) * NX + x for z in range(NZ) for y in range(NY) for x in range(NX)])


def xy_major_groups():
    return np.array([(y * NZ + z) * NX + x for y in range(NY) for x in range(NX) for z in range(NZ)])


def x_table(cells, keep):
    theta = angles(signed(np.arange(keep), keep), np.arange(cells), cells).T
    block = keep // 2
    parts = []
    for h in range(2):
        cut = theta[:, h * block : (h + 1) * block]
        parts += [np.cos(cut), -np.sin(cut)]
    return np.concatenate(halves(np.concatenate(parts, axis=1) / math.sqrt(cells)), axis=0)


def y_table(cells, keep, order):
    modes = signed(np.arange(keep), keep)
    return np.stack(
        [rows_of(angles(modes[parity::2][order], np.arange(cells // 2), cells), cells) for parity in range(2)]
    )


def z_table(cells, keep, positions):
    return rows_of(angles(signed(np.arange(keep), keep), positions, cells), cells)


def split(x):
    high = x.astype(jnp.bfloat16)
    low = (x - high.astype(jnp.float32)).astype(jnp.bfloat16)
    return high, low


def product(a, b):
    return jnp.dot(a, b, preferred_element_type=jnp.float32)


def transformed(high_table, low_table, x):
    high, low = split(x)
    return product(
        jnp.concatenate([high_table, high_table, low_table], axis=1), jnp.concatenate([high, low, high], axis=0)
    )


def place():
    pen = lax.axis_index("pen")
    x = lax.rem(pen, NX)
    z = lax.rem(lax.div(pen, NX), NZ)
    y = lax.axis_index("section") * 2 + lax.div(pen, NX * NZ)
    return y, z, x


def cross_kernel(v_hbm, w_hbm, *refs):
    outs, (v_ref, w_ref, sems) = refs[:-3], refs[-3:]
    rows, cells = v_ref.shape[2:]
    copies = [
        [
            copy
            for c in range(3)
            for copy in (
                pltpu.make_async_copy(v_hbm.at[c, plane], v_ref.at[plane, c], sems.at[plane * 6 + c]),
                pltpu.make_async_copy(w_hbm.at[c, plane], w_ref.at[plane, c], sems.at[plane * 6 + 3 + c]),
            )
        ]
        for plane in range(len(outs))
    ]
    for group in copies:
        for copy in group:
            copy.start()
    for plane, out_ref in enumerate(outs):
        for copy in copies[plane]:
            copy.wait()
        for c in range(3):
            a, b = (c + 1) % 3, (c + 2) % 3
            high, low = split(v_ref[plane, a] * w_ref[plane, b] - v_ref[plane, b] * w_ref[plane, a])
            out_ref[c * rows : (c + 1) * rows, :cells] = high
            out_ref[c * rows : (c + 1) * rows, cells:] = low


def x_kernel(*refs):
    planes, (table_ref, keep_ref, send_ref) = refs[:-3], refs[-3:]
    cells = planes[0].shape[1] // 2
    rows = planes[0].shape[0]
    half = keep_ref.shape[-1]
    mine = lax.axis_index("slab") == 0
    table = jnp.concatenate([table_ref[:cells], table_ref[:cells], table_ref[cells:]], axis=0)
    for i, ref in enumerate(planes):
        both = ref[...]
        out = product(jnp.concatenate([both, both[:, :cells]], axis=1), table)
        first, second = out[:, :half], out[:, half:]
        here = slice(i * rows, (i + 1) * rows)
        keep_ref[here] = jnp.where(mine, first, second)
        send_ref[here] = jnp.where(mine, second, first)


def y_blocks(keep_ref, got_ref, table_ref, rows):
    sign = jnp.where(lax.axis_index("slab") == 0, 1.0, -1.0).astype(jnp.float32)
    dests = table_ref.shape[2] // 2
    lanes = keep_ref.shape[1] // 2
    for block in range(keep_ref.shape[0] // rows):
        here = slice(block * rows, (block + 1) * rows)
        own, got = keep_ref[here], got_ref[here]
        for parity in range(2):
            folded = own + got if parity == 0 else (own - got) * sign
            out = transformed(table_ref[parity, 0], table_ref[parity, 1], folded)
            yield block, parity * 2, out[:dests, :lanes] + out[dests:, lanes:]
            yield block, parity * 2 + 1, out[:dests, lanes:] - out[dests:, :lanes]


def y_pack_kernel(rows, keep_ref, got_ref, table_ref, _, out_ref):
    dests = table_ref.shape[2] // 2
    per = out_ref.shape[0] // dests
    for block, q, value in y_blocks(keep_ref, got_ref, table_ref, rows):
        out_ref[pl.ds(block * 4 + q, dests, per), :] = value


def y_send_kernel(rows, keep_ref, got_ref, table_ref, *refs):
    outs, all_ref = refs[:-1], refs[-1]
    dests = table_ref.shape[2] // 2
    for block, q, value in y_blocks(keep_ref, got_ref, table_ref, rows):
        at = (block * 4 + q) * dests
        all_ref[at : at + dests] = value
    _, z, _ = place()
    for shift in range(NZ):
        to = lax.rem(z - shift + NZ, NZ)
        for k in range(all_ref.shape[0] // dests):
            outs[shift][k * NXY : (k + 1) * NXY] = all_ref[pl.ds(pl.multiple_of(k * dests + to * NXY, NXY), NXY), :]


def turn_kernel(*refs):
    gots, outs, all_ref = refs[:NZ], refs[NZ:-1], refs[-1]
    y, z, x = place()
    size = gots[0].shape[0]
    for shift in range(NZ):
        source = lax.rem(z + shift, NZ)
        all_ref[pl.ds(pl.multiple_of(source * size, size), size), :] = gots[shift][...]
    count = all_ref.shape[0] // NXY
    for dy in range(NY):
        for dx in range(NX):
            to = lax.rem(y - dy + NY, NY) * NX + lax.rem(x - dx + NX, NX)
            outs[dy * NX + dx][...] = all_ref[pl.ds(to, count, NXY), :]


def wave_numbers(keep, lanes, first, count):
    group = lax.axis_index("section") * lax.axis_size("pen") + lax.axis_index("pen")
    limit = -(keep // 2)
    visc = 0.5 / (keep // 2) ** 2
    row = lax.broadcasted_iota(jnp.int32, (count, lanes), 0) + first
    col = lax.broadcasted_iota(jnp.int32, (count, lanes), 1) + lax.axis_index("slab") * lanes
    kz = jnp.where(row < keep // 2, row, row - keep)
    kx = jnp.where(col < keep // 2, col, col - keep)
    for parity in range(2):
        index = group * 2 + parity
        ky = jnp.where(index < keep // 2, index, index - keep)
        mask = ((kx != limit) & (kz != limit) & (ky != limit)).astype(jnp.float32)
        waves = (kx.astype(jnp.float32), ky.astype(jnp.float32), kz.astype(jnp.float32))
        ksq = waves[0] * waves[0] + waves[1] * waves[1] + waves[2] * waves[2]
        yield parity, waves, mask, 1.0 / jnp.maximum(ksq, 1.0), visc * ksq


def projected(s, waves, mask, inverse):
    inner = (waves[0] * s[0] + waves[1] * s[1] + waves[2] * s[2]) * inverse
    return [mask * (s[c] - waves[c] * inner) for c in range(3)]


def z_sums(keep, lanes, table, columns):
    out = transformed(table[0], table[1], columns)
    return out[:keep, :lanes] + out[keep:, lanes:], out[:keep, lanes:] - out[keep:, :lanes]


def early_kernel(keep, *refs):
    gots, (modes_ref, table_ref, out_ref, all_ref) = refs[:NXY], refs[NXY:]
    y, _, x = place()
    lanes = out_ref.shape[1]
    kinds = gots[0].shape[0] // NZ
    sources = NXY * NZ
    for dy in range(NY):
        for dx in range(NX):
            source = lax.rem(y + dy, NY) * NX + lax.rem(x + dx, NX)
            for k in range(kinds):
                at = pl.multiple_of(k * sources + source * NZ, NZ)
                all_ref[pl.ds(at, NZ), :] = gots[dy * NX + dx][pl.ds(k, NZ, kinds), :]
    for parity, waves, mask, inverse, damp in wave_numbers(keep, lanes, 0, keep):
        sums = []
        for c in range(3):
            base = c * 4 + parity * 2
            both = [all_ref[(base + q) * sources : (base + q + 1) * sources] for q in range(2)]
            sums.append(z_sums(keep, lanes, table_ref, jnp.concatenate(both, axis=1)))
        for q in range(2):
            for c, value in enumerate(projected([s[q] for s in sums], waves, mask, inverse)):
                where = pl.ds(c * keep * 4 + parity * 2 + q, keep, 4)
                out_ref[where, :] = value - damp * modes_ref[where, :]


def z_kernel(planes, keep, x_ref, early_ref, table_ref, out_hbm, sums_ref, out_ref, sems):
    lanes = x_ref.shape[1]
    per = 3 * planes * 4
    sources = x_ref.shape[0] // per
    for parity in range(2):
        for c in range(3):
            columns = [
                jnp.concatenate(
                    [x_ref[pl.ds((p * 3 + c) * 4 + parity * 2 + q, sources, per), :] for p in range(planes)], axis=0
                )
                for q in range(2)
            ]
            pair = z_sums(keep, lanes, table_ref, jnp.concatenate(columns, axis=1))
            for q in range(2):
                sums_ref[parity, q, c] = pair[q]
    count = sems.shape[0] // 3
    part = keep // count
    copies = []
    for h in range(count):
        here = slice(h * part, (h + 1) * part)
        for parity, waves, mask, inverse, _ in wave_numbers(keep, lanes, h * part, part):
            for q in range(2):
                values = projected([sums_ref[parity, q, c, here] for c in range(3)], waves, mask, inverse)
                for c, value in enumerate(values):
                    where = pl.ds((c * keep + h * part) * 4 + parity * 2 + q, part, 4)
                    out_ref[where, :] = value + early_ref[where, :]
        for c in range(3):
            rows = pl.ds((c * keep + h * part) * 4, part * 4)
            copies.append(pltpu.make_async_copy(out_ref.at[rows], out_hbm.at[rows], sems.at[h * 3 + c]))
            copies[-1].start()
    for copy in copies:
        copy.wait()


def call(kernel, outs, flops=0, scratch=(), space=VMEM, out_space=VMEM, limit=40 << 20, kind=jnp.float32):
    def run(*args):
        size = sum(a.size * a.dtype.itemsize for a in args) + sum(4 * math.prod(o) for o in outs)
        shapes = [jax.ShapeDtypeStruct(o, kind) for o in outs]
        specs = [pl.BlockSpec(memory_space=out_space)] * len(outs)
        single = len(outs) == 1
        return pl.pallas_call(
            kernel,
            out_shape=shapes[0] if single else shapes,
            in_specs=[pl.BlockSpec(memory_space=space)] * len(args),
            out_specs=specs[0] if single else specs,
            scratch_shapes=list(scratch),
            cost_estimate=pl.CostEstimate(flops=flops, bytes_accessed=size, transcendentals=0),
            compiler_params=pltpu.CompilerParams(vmem_limit_bytes=limit),
        )(*args)

    return run


def group_of(y, z, x):
    return ((y % NY) * NZ + z % NZ) * NX + x % NX


def from_shift(value, dy, dz, dx):
    pairs = [
        (group_of(y + dy, z + dz, x + dx), group_of(y, z, x))
        for y in range(NY)
        for z in range(NZ)
        for x in range(NX)
    ]
    return lax.ppermute(value, GROUP, pairs)


def per_device(velocity, vorticity, velocity_modes):
    _, planes, rows_y, cells = velocity.shape
    _, keep, rows_ky, _, lanes = velocity_modes.shape
    dests = lax.axis_size(GROUP)
    order = z_major_groups()
    table_y = jnp.asarray(y_table(cells, keep, order))
    table_x = jnp.asarray(x_table(cells, keep))
    crosses = call(
        cross_kernel,
        [(3 * rows_y, 2 * cells)] * planes,
        6 * planes * 3 * rows_y * cells,
        [VMEM((planes, 3, rows_y, cells), jnp.float32)] * 2 + [pltpu.SemaphoreType.DMA((6 * planes,))],
        pltpu.HBM,
        limit=50 << 20,
        kind=jnp.bfloat16,
    )(velocity, vorticity)
    keeps, gots = [], []
    for held in (crosses[:1], crosses[1:]):
        n = len(held)
        run = call(x_kernel, [(3 * n * rows_y, keep)] * 2, 2 * 9 * n * rows_y * cells * 2 * keep)
        mine, other = run(*held, table_x)
        keeps.append(mine)
        gots.append(lax.ppermute(other, "slab", [(0, 1), (1, 0)]))
    flops = 2 * 3 * 2 * keep * 3 * rows_y * keep
    kinds = 3 * 4
    sent = call(
        functools.partial(y_send_kernel, rows_y),
        [(kinds * NXY, lanes)] * NZ,
        flops,
        [VMEM((kinds * dests, lanes), jnp.float32)],
    )(keeps[0], gots[0], table_y)
    arrived = [sent[0]]
    for s in range(1, NZ):
        arrived.append(from_shift(sent[s], 0, s, 0))
    per = (planes - 1) * kinds
    packed = call(
        functools.partial(y_pack_kernel, rows_y), [(dests * per, lanes)], flops * (planes - 1)
    )(keeps[1], gots[1], table_y, sent[0])
    late = lax.all_to_all(
        packed.reshape(dests, per, lanes), GROUP, 0, 0, axis_index_groups=[order.tolist()], tiled=True
    )
    turned = call(turn_kernel, [(NZ * kinds, lanes)] * NXY, 0, [VMEM((NZ * kinds * NXY, lanes), jnp.float32)])(*arrived)
    spread = [turned[0]] + [from_shift(turned[d], d // NX, 0, d % NX) for d in range(1, NXY)]
    early = call(
        functools.partial(early_kernel, keep),
        [(3 * keep * 4, lanes)],
        2 * 6 * 2 * keep * 3 * dests * keep,
        [VMEM((kinds * dests, lanes), jnp.float32)],
    )(
        *spread,
        velocity_modes.reshape(3 * keep * 4, lanes),
        jnp.asarray(z_table(cells, keep, planes * xy_major_groups())),
    )
    rest = np.concatenate([planes * order + p for p in range(1, planes)])
    table_z = jnp.asarray(z_table(cells, keep, rest))
    out = call(
        functools.partial(z_kernel, planes - 1, keep),
        [(3 * keep * 4, lanes)],
        2 * 6 * 2 * keep * 3 * (planes - 1) * dests * keep,
        [
            VMEM((2, 2, 3, keep, lanes), jnp.float32),
            VMEM((3 * keep * 4, lanes), jnp.float32),
            pltpu.SemaphoreType.DMA((6,)),
        ],
        out_space=pltpu.HBM,
    )(late.reshape(dests * per, lanes), early, table_z)
    return out.reshape(3, keep, rows_ky, 2, lanes)


def solution(mesh):
    return jax.shard_map(
        per_device,
        mesh=mesh,
        in_specs=(
            P(None, GROUP, "slab", None),
            P(None, GROUP, "slab", None),
            P(None, None, GROUP, None, "slab"),
        ),
        out_specs=P(None, None, GROUP, None, "slab"),
        check_vma=False,
    )
```

```python
import functools
import math

import jax
import jax.numpy as jnp
import ml_dtypes
import numpy as np
from jax import lax
from jax.experimental import pallas as pl
from jax.experimental.pallas import tpu as pltpu
from jax.sharding import PartitionSpec as P

VMEM = pltpu.VMEM
GROUP = ("section", "pen")
NY, NZ, NX = 4, 8, 4
NXY = NX * NY


def signed(index, count):
    return np.where(index < count // 2, index, index - count)


def halves(table):
    high = table.astype(np.float32).astype(ml_dtypes.bfloat16)
    low = (table - high.astype(np.float64)).astype(np.float32).astype(ml_dtypes.bfloat16)
    return high, low


def angles(modes, positions, length):
    return 2.0 * math.pi / length * ((modes[:, None] * positions[None, :]) % length)


def rows_of(theta, cells):
    return np.stack(halves(np.concatenate([np.cos(theta), np.sin(theta)], axis=0) / math.sqrt(cells)))


def z_major_groups():
    return np.array([(y * NZ + z) * NX + x for z in range(NZ) for y in range(NY) for x in range(NX)])


def xy_major_groups():
    return np.array([(y * NZ + z) * NX + x for y in range(NY) for x in range(NX) for z in range(NZ)])


def x_table(cells, keep):
    theta = angles(signed(np.arange(keep), keep), np.arange(cells), cells).T
    block = keep // 2
    parts = []
    for h in range(2):
        cut = theta[:, h * block : (h + 1) * block]
        parts += [np.cos(cut), -np.sin(cut)]
    return np.concatenate(halves(np.concatenate(parts, axis=1) / math.sqrt(cells)), axis=0)


def y_table(cells, keep, order):
    modes = signed(np.arange(keep), keep)
    return np.stack(
        [rows_of(angles(modes[parity::2][order], np.arange(cells // 2), cells), cells) for parity in range(2)]
    )


def folded_z_table(cells, keep, positions):
    modes = signed(np.arange(keep), keep)
    return np.stack([rows_of(angles(modes[parity::2], positions, cells), cells) for parity in range(2)])


def z_table(cells, keep, positions):
    return rows_of(angles(signed(np.arange(keep), keep), positions, cells), cells)


def split(x):
    high = x.astype(jnp.bfloat16)
    low = (x - high.astype(jnp.float32)).astype(jnp.bfloat16)
    return high, low


def product(a, b):
    return jnp.dot(a, b, preferred_element_type=jnp.float32)


def transformed(high_table, low_table, x):
    high, low = split(x)
    return product(
        jnp.concatenate([high_table, high_table, low_table], axis=1), jnp.concatenate([high, low, high], axis=0)
    )


def place():
    pen = lax.axis_index("pen")
    x = lax.rem(pen, NX)
    z = lax.rem(lax.div(pen, NX), NZ)
    y = lax.axis_index("section") * 2 + lax.div(pen, NX * NZ)
    return y, z, x


def cross_kernel(v_hbm, w_hbm, *refs):
    outs, (v_ref, w_ref, sems) = refs[:-3], refs[-3:]
    rows, cells = v_ref.shape[2:]
    copies = [
        [
            copy
            for c in range(3)
            for copy in (
                pltpu.make_async_copy(v_hbm.at[c, plane], v_ref.at[plane, c], sems.at[plane * 6 + c]),
                pltpu.make_async_copy(w_hbm.at[c, plane], w_ref.at[plane, c], sems.at[plane * 6 + 3 + c]),
            )
        ]
        for plane in range(len(outs))
    ]
    for group in copies:
        for copy in group:
            copy.start()
    for plane, out_ref in enumerate(outs):
        for copy in copies[plane]:
            copy.wait()
        for c in range(3):
            a, b = (c + 1) % 3, (c + 2) % 3
            high, low = split(v_ref[plane, a] * w_ref[plane, b] - v_ref[plane, b] * w_ref[plane, a])
            out_ref[c * rows : (c + 1) * rows, :cells] = high
            out_ref[c * rows : (c + 1) * rows, cells:] = low


def x_kernel(*refs):
    planes, (table_ref, keep_ref, send_ref) = refs[:-3], refs[-3:]
    cells = planes[0].shape[1] // 2
    rows = planes[0].shape[0]
    half = keep_ref.shape[-1]
    mine = lax.axis_index("slab") == 0
    table = jnp.concatenate([table_ref[:cells], table_ref[:cells], table_ref[cells:]], axis=0)
    for i, ref in enumerate(planes):
        both = ref[...]
        out = product(jnp.concatenate([both, both[:, :cells]], axis=1), table)
        first, second = out[:, :half], out[:, half:]
        here = slice(i * rows, (i + 1) * rows)
        keep_ref[here] = jnp.where(mine, first, second)
        send_ref[here] = jnp.where(mine, second, first)


def y_blocks(keep_ref, got_ref, table_ref, rows):
    sign = jnp.where(lax.axis_index("slab") == 0, 1.0, -1.0).astype(jnp.float32)
    dests = table_ref.shape[2] // 2
    lanes = keep_ref.shape[1] // 2
    for block in range(keep_ref.shape[0] // rows):
        here = slice(block * rows, (block + 1) * rows)
        own, got = keep_ref[here], got_ref[here]
        for parity in range(2):
            folded = own + got if parity == 0 else (own - got) * sign
            out = transformed(table_ref[parity, 0], table_ref[parity, 1], folded)
            yield block, parity * 2, out[:dests, :lanes] + out[dests:, lanes:]
            yield block, parity * 2 + 1, out[:dests, lanes:] - out[dests:, :lanes]


def y_pack_kernel(rows, keep_ref, got_ref, table_ref, _, out_ref):
    dests = table_ref.shape[2] // 2
    per = out_ref.shape[0] // dests
    for block, q, value in y_blocks(keep_ref, got_ref, table_ref, rows):
        out_ref[pl.ds(block * 4 + q, dests, per), :] = value


def y_send_kernel(rows, keep_ref, got_ref, table_ref, *refs):
    outs, all_ref = refs[:-1], refs[-1]
    dests = table_ref.shape[2] // 2
    for block, q, value in y_blocks(keep_ref, got_ref, table_ref, rows):
        at = (block * 4 + q) * dests
        all_ref[at : at + dests] = value
    _, z, _ = place()
    for shift in range(NZ):
        to = lax.rem(z - shift + NZ, NZ)
        for k in range(all_ref.shape[0] // dests):
            outs[shift][k * NXY : (k + 1) * NXY] = all_ref[pl.ds(pl.multiple_of(k * dests + to * NXY, NXY), NXY), :]


def turn_kernel(*refs):
    gots, outs, all_ref = refs[:NZ], refs[NZ:-1], refs[-1]
    y, z, x = place()
    size = gots[0].shape[0]
    for shift in range(NZ):
        source = lax.rem(z + shift, NZ)
        all_ref[pl.ds(pl.multiple_of(source * size, size), size), :] = gots[shift][...]
    count = all_ref.shape[0] // NXY
    for dy in range(NY):
        for dx in range(NX):
            to = lax.rem(y - dy + NY, NY) * NX + lax.rem(x - dx + NX, NX)
            outs[dy * NX + dx][...] = all_ref[pl.ds(to, count, NXY), :]


def wave_numbers(keep, lanes, first, count, step):
    group = lax.axis_index("section") * lax.axis_size("pen") + lax.axis_index("pen")
    limit = -(keep // 2)
    visc = 0.5 / (keep // 2) ** 2
    row = lax.broadcasted_iota(jnp.int32, (count, lanes), 0) * step + first
    col = lax.broadcasted_iota(jnp.int32, (count, lanes), 1) + lax.axis_index("slab") * lanes
    kz = jnp.where(row < keep // 2, row, row - keep)
    kx = jnp.where(col < keep // 2, col, col - keep)
    for parity in range(2):
        index = group * 2 + parity
        ky = jnp.where(index < keep // 2, index, index - keep)
        mask = ((kx != limit) & (kz != limit) & (ky != limit)).astype(jnp.float32)
        waves = (kx.astype(jnp.float32), ky.astype(jnp.float32), kz.astype(jnp.float32))
        ksq = waves[0] * waves[0] + waves[1] * waves[1] + waves[2] * waves[2]
        yield parity, waves, mask, 1.0 / jnp.maximum(ksq, 1.0), visc * ksq


def projected(s, waves, mask, inverse):
    inner = (waves[0] * s[0] + waves[1] * s[1] + waves[2] * s[2]) * inverse
    return [mask * (s[c] - waves[c] * inner) for c in range(3)]


def z_sums(keep, lanes, table, columns):
    out = transformed(table[0], table[1], columns)
    return out[:keep, :lanes] + out[keep:, lanes:], out[:keep, lanes:] - out[keep:, :lanes]


def early_kernel(keep, *refs):
    gots, (modes_hbm, table_ref, out_ref, all_ref, modes_ref, sem) = refs[:NXY], refs[NXY:]
    copy = pltpu.make_async_copy(modes_hbm, modes_ref, sem)
    copy.start()
    y, _, x = place()
    lanes = out_ref.shape[1]
    kinds = gots[0].shape[0] // NZ
    sources = NXY * NZ
    for dy in range(NY):
        for dx in range(NX):
            source = lax.rem(y + dy, NY) * NX + lax.rem(x + dx, NX)
            for k in range(kinds):
                at = pl.multiple_of(k * sources + source * NZ, NZ)
                all_ref[pl.ds(at, NZ), :] = gots[dy * NX + dx][pl.ds(k, NZ, kinds), :]
    copy.wait()
    for parity, waves, mask, inverse, damp in wave_numbers(keep, lanes, 0, keep, 1):
        sums = []
        for c in range(3):
            base = c * 4 + parity * 2
            both = [all_ref[(base + q) * sources : (base + q + 1) * sources] for q in range(2)]
            sums.append(z_sums(keep, lanes, table_ref, jnp.concatenate(both, axis=1)))
        for q in range(2):
            for c, value in enumerate(projected([s[q] for s in sums], waves, mask, inverse)):
                where = pl.ds(c * keep * 4 + parity * 2 + q, keep, 4)
                out_ref[where, :] = value - damp * modes_ref[where, :]


def z_kernel(planes, keep, x_ref, early_ref, table_ref, out_hbm, sums_ref, out_ref, sems):
    lanes = x_ref.shape[1]
    per = 3 * planes * 4
    sources = x_ref.shape[0] // per
    run = NXY // 2
    for parity in range(2):
        for c in range(3):
            sums, differences = [], []
            for p in range(planes):
                at = (p * 3 + c) * 4 + parity * 2
                both = jnp.concatenate([x_ref[pl.ds(at + q, sources, per), :] for q in range(2)], axis=1)
                both = both.reshape(NZ, 2, run, 2 * lanes)
                sums.append((both[:, 0] + both[:, 1]).reshape(NZ * run, 2 * lanes))
                differences.append((both[:, 0] - both[:, 1]).reshape(NZ * run, 2 * lanes))
            for e, folded in enumerate((sums, differences)):
                pair = z_sums(keep // 2, lanes, table_ref.at[e], jnp.concatenate(folded, axis=0))
                for q in range(2):
                    sums_ref[parity, q, c, e] = pair[q]
    count = sems.shape[0] // 3
    part = keep // 2 // count
    copies = []
    for h in range(count):
        here = slice(h * part, (h + 1) * part)
        for e in range(2):
            for parity, waves, mask, inverse, _ in wave_numbers(keep, lanes, h * part * 2 + e, part, 2):
                for q in range(2):
                    values = projected([sums_ref[parity, q, c, e, here] for c in range(3)], waves, mask, inverse)
                    for c, value in enumerate(values):
                        where = pl.ds((c * keep + h * part * 2 + e) * 4 + parity * 2 + q, part, 8)
                        out_ref[where, :] = value + early_ref[where, :]
        for c in range(3):
            rows = pl.ds((c * keep + h * part * 2) * 4, part * 8)
            copies.append(pltpu.make_async_copy(out_ref.at[rows], out_hbm.at[rows], sems.at[h * 3 + c]))
            copies[-1].start()
    for copy in copies:
        copy.wait()


def call(kernel, outs, flops=0, scratch=(), space=VMEM, out_space=VMEM, limit=40 << 20, kind=jnp.float32):
    def run(*args):
        size = sum(a.size * a.dtype.itemsize for a in args) + sum(4 * math.prod(o) for o in outs)
        shapes = [jax.ShapeDtypeStruct(o, kind) for o in outs]
        specs = [pl.BlockSpec(memory_space=out_space)] * len(outs)
        single = len(outs) == 1
        return pl.pallas_call(
            kernel,
            out_shape=shapes[0] if single else shapes,
            in_specs=[pl.BlockSpec(memory_space=m) for m in (space if isinstance(space, list) else [space] * len(args))],
            out_specs=specs[0] if single else specs,
            scratch_shapes=list(scratch),
            cost_estimate=pl.CostEstimate(flops=flops, bytes_accessed=size, transcendentals=0),
            compiler_params=pltpu.CompilerParams(vmem_limit_bytes=limit),
        )(*args)

    return run


def group_of(y, z, x):
    return ((y % NY) * NZ + z % NZ) * NX + x % NX


def from_shift(value, dy, dz, dx):
    pairs = [
        (group_of(y + dy, z + dz, x + dx), group_of(y, z, x))
        for y in range(NY)
        for z in range(NZ)
        for x in range(NX)
    ]
    return lax.ppermute(value, GROUP, pairs)


def per_device(velocity, vorticity, velocity_modes):
    _, planes, rows_y, cells = velocity.shape
    _, keep, rows_ky, _, lanes = velocity_modes.shape
    dests = lax.axis_size(GROUP)
    order = z_major_groups()
    table_y = jnp.asarray(y_table(cells, keep, order))
    table_x = jnp.asarray(x_table(cells, keep))
    crosses = call(
        cross_kernel,
        [(3 * rows_y, 2 * cells)] * planes,
        6 * planes * 3 * rows_y * cells,
        [VMEM((planes, 3, rows_y, cells), jnp.float32)] * 2 + [pltpu.SemaphoreType.DMA((6 * planes,))],
        pltpu.HBM,
        limit=50 << 20,
        kind=jnp.bfloat16,
    )(velocity, vorticity)
    keeps, gots = [], []
    for held in (crosses[:1], crosses[1:]):
        n = len(held)
        run = call(x_kernel, [(3 * n * rows_y, keep)] * 2, 2 * 9 * n * rows_y * cells * 2 * keep)
        mine, other = run(*held, table_x)
        keeps.append(mine)
        gots.append(lax.ppermute(other, "slab", [(0, 1), (1, 0)]))
    flops = 2 * 3 * 2 * keep * 3 * rows_y * keep
    kinds = 3 * 4
    sent = call(
        functools.partial(y_send_kernel, rows_y),
        [(kinds * NXY, lanes)] * NZ,
        flops,
        [VMEM((kinds * dests, lanes), jnp.float32)],
    )(keeps[0], gots[0], table_y)
    arrived = [sent[0]]
    for s in range(1, NZ):
        arrived.append(from_shift(sent[s], 0, s, 0))
    per = (planes - 1) * kinds
    packed = call(
        functools.partial(y_pack_kernel, rows_y), [(dests * per, lanes)], flops * (planes - 1)
    )(keeps[1], gots[1], table_y, sent[0])
    late = lax.all_to_all(
        packed.reshape(dests, per, lanes), GROUP, 0, 0, axis_index_groups=[order.tolist()], tiled=True
    )
    turned = call(turn_kernel, [(NZ * kinds, lanes)] * NXY, 0, [VMEM((NZ * kinds * NXY, lanes), jnp.float32)])(*arrived)
    spread = [turned[0]] + [from_shift(turned[d], d // NX, 0, d % NX) for d in range(1, NXY)]
    early = call(
        functools.partial(early_kernel, keep),
        [(3 * keep * 4, lanes)],
        2 * 6 * 2 * keep * 3 * dests * keep,
        [
            VMEM((kinds * dests, lanes), jnp.float32),
            VMEM((3 * keep * 4, lanes), jnp.float32),
            pltpu.SemaphoreType.DMA,
        ],
        [VMEM] * NXY + [pltpu.HBM, VMEM],
        limit=50 << 20,
    )(
        *spread,
        velocity_modes.reshape(3 * keep * 4, lanes),
        jnp.asarray(z_table(cells, keep, planes * xy_major_groups())),
    )
    near = order.reshape(NZ, 2, -1)[:, 0].reshape(-1)
    rest = np.concatenate([planes * near + p for p in range(1, planes)])
    table_z = jnp.asarray(folded_z_table(cells, keep, rest))
    out = call(
        functools.partial(z_kernel, planes - 1, keep),
        [(3 * keep * 4, lanes)],
        6 * 2 * keep * 3 * (planes - 1) * dests * keep,
        [
            VMEM((2, 2, 3, 2, keep // 2, lanes), jnp.float32),
            VMEM((3 * keep * 4, lanes), jnp.float32),
            pltpu.SemaphoreType.DMA((6,)),
        ],
        out_space=pltpu.HBM,
    )(late.reshape(dests * per, lanes), early, table_z)
    return out.reshape(3, keep, rows_ky, 2, lanes)


def solution(mesh):
    return jax.shard_map(
        per_device,
        mesh=mesh,
        in_specs=(
            P(None, GROUP, "slab", None),
            P(None, GROUP, "slab", None),
            P(None, None, GROUP, None, "slab"),
        ),
        out_specs=P(None, None, GROUP, None, "slab"),
        check_vma=False,
    )
```

```python
import functools
import math

import jax
import jax.numpy as jnp
import ml_dtypes
import numpy as np
from jax import lax
from jax.experimental import pallas as pl
from jax.experimental.pallas import tpu as pltpu
from jax.sharding import PartitionSpec as P

VMEM = pltpu.VMEM
GROUP = ("section", "pen")
NY, NZ, NX = 4, 8, 4
NXY = NX * NY
EARLY = 4


def signed(index, count):
    return np.where(index < count // 2, index, index - count)


def halves(table):
    high = table.astype(np.float32).astype(ml_dtypes.bfloat16)
    low = (table - high.astype(np.float64)).astype(np.float32).astype(ml_dtypes.bfloat16)
    return high, low


def angles(modes, positions, length):
    return 2.0 * math.pi / length * ((modes[:, None] * positions[None, :]) % length)


def rows_of(theta, cells):
    return np.stack(halves(np.concatenate([np.cos(theta), np.sin(theta)], axis=0) / math.sqrt(cells)))


def z_major_groups():
    return np.array([(y * NZ + z) * NX + x for z in range(NZ) for y in range(NY) for x in range(NX)])


def xy_major_groups():
    return np.array([(y * NZ + z) * NX + x for y in range(NY) for x in range(NX) for z in range(NZ)])


def x_table(cells, keep):
    theta = angles(signed(np.arange(keep), keep), np.arange(cells), cells).T
    block = keep // 2
    parts = []
    for h in range(2):
        cut = theta[:, h * block : (h + 1) * block]
        parts += [np.cos(cut), -np.sin(cut)]
    return np.concatenate(halves(np.concatenate(parts, axis=1) / math.sqrt(cells)), axis=0)


def y_table(cells, keep, order):
    modes = signed(np.arange(keep), keep)
    return np.stack(
        [rows_of(angles(modes[parity::2][order], np.arange(cells // 2), cells), cells) for parity in range(2)]
    )


def folded_z_table(cells, keep, positions):
    modes = signed(np.arange(keep), keep)
    return np.stack([rows_of(angles(modes[parity::2], positions, cells), cells) for parity in range(2)])


def split(x):
    high = x.astype(jnp.bfloat16)
    low = (x - high.astype(jnp.float32)).astype(jnp.bfloat16)
    return high, low


def product(a, b):
    return jnp.dot(a, b, preferred_element_type=jnp.float32)


def transformed(high_table, low_table, x):
    high, low = split(x)
    return product(
        jnp.concatenate([high_table, high_table, low_table], axis=1), jnp.concatenate([high, low, high], axis=0)
    )


def place():
    pen = lax.axis_index("pen")
    x = lax.rem(pen, NX)
    z = lax.rem(lax.div(pen, NX), NZ)
    y = lax.axis_index("section") * 2 + lax.div(pen, NX * NZ)
    return y, z, x


def cross_kernel(v_hbm, w_hbm, *refs):
    outs, (v_ref, w_ref, sems) = refs[:-3], refs[-3:]
    rows, cells = v_ref.shape[2:]
    copies = [
        [
            copy
            for c in range(3)
            for copy in (
                pltpu.make_async_copy(v_hbm.at[c, plane], v_ref.at[plane, c], sems.at[plane * 6 + c]),
                pltpu.make_async_copy(w_hbm.at[c, plane], w_ref.at[plane, c], sems.at[plane * 6 + 3 + c]),
            )
        ]
        for plane in range(len(outs))
    ]
    for group in copies:
        for copy in group:
            copy.start()
    for plane, out_ref in enumerate(outs):
        for copy in copies[plane]:
            copy.wait()
        for c in range(3):
            a, b = (c + 1) % 3, (c + 2) % 3
            high, low = split(v_ref[plane, a] * w_ref[plane, b] - v_ref[plane, b] * w_ref[plane, a])
            out_ref[c * rows : (c + 1) * rows, :cells] = high
            out_ref[c * rows : (c + 1) * rows, cells:] = low


def x_kernel(spans, *refs):
    inputs, (table_ref, keep_ref, send_ref) = refs[:-3], refs[-3:]
    cells = inputs[0].shape[1] // 2
    half = keep_ref.shape[-1]
    mine = lax.axis_index("slab") == 0
    table = jnp.concatenate([table_ref[:cells], table_ref[:cells], table_ref[cells:]], axis=0)
    at = 0
    for ref, (first_row, last_row) in zip(inputs, spans):
        both = ref[first_row:last_row]
        out = product(jnp.concatenate([both, both[:, :cells]], axis=1), table)
        first, second = out[:, :half], out[:, half:]
        here = slice(at, at + last_row - first_row)
        keep_ref[here] = jnp.where(mine, first, second)
        send_ref[here] = jnp.where(mine, second, first)
        at += last_row - first_row


def y_blocks(keep_ref, got_ref, table_ref, rows):
    sign = jnp.where(lax.axis_index("slab") == 0, 1.0, -1.0).astype(jnp.float32)
    dests = table_ref.shape[2] // 2
    lanes = keep_ref.shape[1] // 2
    for block in range(keep_ref.shape[0] // rows):
        here = slice(block * rows, (block + 1) * rows)
        own, got = keep_ref[here], got_ref[here]
        for parity in range(2):
            folded = own + got if parity == 0 else (own - got) * sign
            out = transformed(table_ref[parity, 0], table_ref[parity, 1], folded)
            yield block, parity * 2, out[:dests, :lanes] + out[dests:, lanes:]
            yield block, parity * 2 + 1, out[:dests, lanes:] - out[dests:, :lanes]


def y_pack_kernel(rows, keep_ref, got_ref, table_ref, _, out_ref):
    dests = table_ref.shape[2] // 2
    per = out_ref.shape[0] // dests
    for block, q, value in y_blocks(keep_ref, got_ref, table_ref, rows):
        out_ref[pl.ds(block * 4 + q, dests, per), :] = value


def y_send_kernel(rows, keep_ref, got_ref, table_ref, *refs):
    outs, all_ref = refs[:-1], refs[-1]
    dests = table_ref.shape[2] // 2
    for block, q, value in y_blocks(keep_ref, got_ref, table_ref, rows):
        at = (block * 4 + q) * dests
        all_ref[at : at + dests] = value
    _, z, _ = place()
    for shift in range(NZ):
        to = lax.rem(z - shift + NZ, NZ)
        for k in range(all_ref.shape[0] // dests):
            outs[shift][k * NXY : (k + 1) * NXY] = all_ref[pl.ds(pl.multiple_of(k * dests + to * NXY, NXY), NXY), :]


def turn_kernel(*refs):
    gots, outs, all_ref = refs[:NZ], refs[NZ:-1], refs[-1]
    y, z, x = place()
    size = gots[0].shape[0]
    for shift in range(NZ):
        source = lax.rem(z + shift, NZ)
        all_ref[pl.ds(pl.multiple_of(source * size, size), size), :] = gots[shift][...]
    count = all_ref.shape[0] // NXY
    for dy in range(NY):
        for dx in range(NX):
            to = lax.rem(y - dy + NY, NY) * NX + lax.rem(x - dx + NX, NX)
            outs[dy * NX + dx][...] = all_ref[pl.ds(to, count, NXY), :]


def wave_numbers(keep, lanes, first, count, step):
    group = lax.axis_index("section") * lax.axis_size("pen") + lax.axis_index("pen")
    limit = -(keep // 2)
    visc = 0.5 / (keep // 2) ** 2
    row = lax.broadcasted_iota(jnp.int32, (count, lanes), 0) * step + first
    col = lax.broadcasted_iota(jnp.int32, (count, lanes), 1) + lax.axis_index("slab") * lanes
    kz = jnp.where(row < keep // 2, row, row - keep)
    kx = jnp.where(col < keep // 2, col, col - keep)
    for parity in range(2):
        index = group * 2 + parity
        ky = jnp.where(index < keep // 2, index, index - keep)
        mask = ((kx != limit) & (kz != limit) & (ky != limit)).astype(jnp.float32)
        waves = (kx.astype(jnp.float32), ky.astype(jnp.float32), kz.astype(jnp.float32))
        ksq = waves[0] * waves[0] + waves[1] * waves[1] + waves[2] * waves[2]
        yield parity, waves, mask, 1.0 / jnp.maximum(ksq, 1.0), visc * ksq


def z_sums(keep, lanes, table, columns):
    depth = columns.shape[0]
    out = transformed(table[0, :, :depth], table[1, :, :depth], columns)
    return out[:keep, :lanes] + out[keep:, lanes:], out[:keep, lanes:] - out[keep:, :lanes]


def project_out(keep, lanes, sums_ref, start, count, put):
    for e in range(2):
        for parity, waves, mask, inverse, damp in wave_numbers(keep, lanes, start * 2 + e, count, 2):
            for q in range(2):
                s = [sums_ref[parity, q, c, e, start : start + count] for c in range(3)]
                inner = (waves[0] * s[0] + waves[1] * s[1] + waves[2] * s[2]) * inverse
                for c in range(3):
                    where = pl.ds((c * keep + start * 2 + e) * 4 + parity * 2 + q, count, 8)
                    put(where, mask * (s[c] - waves[c] * inner), damp)


def early_kernel(keep, units, *refs):
    gots, (modes_hbm, table_ref, out_ref, all_ref, sums_ref, modes_ref, sem) = refs[:NXY], refs[NXY:]
    copy = pltpu.make_async_copy(modes_hbm, modes_ref, sem)
    copy.start()
    y, _, x = place()
    lanes = out_ref.shape[1]
    kinds = gots[0].shape[0] // NZ
    sources = NXY * NZ
    for dy in range(NY):
        for dx in range(NX):
            source = lax.rem(y + dy, NY) * NX + lax.rem(x + dx, NX)
            for k in range(kinds):
                at = pl.multiple_of(k * sources + source * NZ, NZ)
                all_ref[pl.ds(at, NZ), :] = gots[dy * NX + dx][pl.ds(k, NZ, kinds), :]
    near = sources // 2
    for parity in range(2):
        for c in range(3):
            folded = [[], []]
            for unit in units[c]:
                base = [(unit * 4 + parity * 2 + q) * sources for q in range(2)]
                one = jnp.concatenate([all_ref[b : b + near] for b in base], axis=1)
                two = jnp.concatenate([all_ref[b + near : b + sources] for b in base], axis=1)
                folded[0].append(one + two)
                folded[1].append(one - two)
            for e in range(2):
                pair = z_sums(keep // 2, lanes, table_ref.at[e], jnp.concatenate(folded[e], axis=0))
                for q in range(2):
                    sums_ref[parity, q, c, e] = pair[q]
    copy.wait()

    def put(where, value, damp):
        out_ref[where, :] = value - damp * modes_ref[where, :]

    project_out(keep, lanes, sums_ref, 0, keep // 2, put)


def z_kernel(keep, units, x_ref, early_ref, table_ref, out_hbm, sums_ref, out_ref, sems):
    lanes = x_ref.shape[1]
    sources = NXY * NZ
    per = x_ref.shape[0] // sources
    run = NXY // 2
    for parity in range(2):
        for c in range(3):
            folded = [[], []]
            for unit in units[c]:
                at = unit * 4 + parity * 2
                both = jnp.concatenate([x_ref[pl.ds(at + q, sources, per), :] for q in range(2)], axis=1)
                both = both.reshape(NZ, 2, run, 2 * lanes)
                folded[0].append((both[:, 0] + both[:, 1]).reshape(NZ * run, 2 * lanes))
                folded[1].append((both[:, 0] - both[:, 1]).reshape(NZ * run, 2 * lanes))
            for e in range(2):
                pair = z_sums(keep // 2, lanes, table_ref.at[e], jnp.concatenate(folded[e], axis=0))
                for q in range(2):
                    sums_ref[parity, q, c, e] = pair[q]

    def put(where, value, damp):
        out_ref[where, :] = value + early_ref[where, :]

    count = sems.shape[0] // 3
    part = keep // 2 // count
    copies = []
    for h in range(count):
        project_out(keep, lanes, sums_ref, h * part, part, put)
        for c in range(3):
            rows = pl.ds((c * keep + h * part * 2) * 4, part * 8)
            copies.append(pltpu.make_async_copy(out_ref.at[rows], out_hbm.at[rows], sems.at[h * 3 + c]))
            copies[-1].start()
    for copy in copies:
        copy.wait()


def call(kernel, outs, flops=0, scratch=(), space=VMEM, out_space=VMEM, limit=40 << 20, kind=jnp.float32):
    def run(*args):
        size = sum(a.size * a.dtype.itemsize for a in args) + sum(4 * math.prod(o) for o in outs)
        shapes = [jax.ShapeDtypeStruct(o, kind) for o in outs]
        specs = [pl.BlockSpec(memory_space=out_space)] * len(outs)
        single = len(outs) == 1
        return pl.pallas_call(
            kernel,
            out_shape=shapes[0] if single else shapes,
            in_specs=[pl.BlockSpec(memory_space=m) for m in (space if isinstance(space, list) else [space] * len(args))],
            out_specs=specs[0] if single else specs,
            scratch_shapes=list(scratch),
            cost_estimate=pl.CostEstimate(flops=flops, bytes_accessed=size, transcendentals=0),
            compiler_params=pltpu.CompilerParams(vmem_limit_bytes=limit),
        )(*args)

    return run


def group_of(y, z, x):
    return ((y % NY) * NZ + z % NZ) * NX + x % NX


def from_shift(value, dy, dz, dx):
    pairs = [
        (group_of(y + dy, z + dz, x + dx), group_of(y, z, x))
        for y in range(NY)
        for z in range(NZ)
        for x in range(NX)
    ]
    return lax.ppermute(value, GROUP, pairs)


def per_device(velocity, vorticity, velocity_modes):
    _, planes, rows_y, cells = velocity.shape
    _, keep, rows_ky, _, lanes = velocity_modes.shape
    dests = lax.axis_size(GROUP)
    order = z_major_groups()
    table_y = jnp.asarray(y_table(cells, keep, order))
    table_x = jnp.asarray(x_table(cells, keep))
    crosses = call(
        cross_kernel,
        [(3 * rows_y, 2 * cells)] * planes,
        6 * planes * 3 * rows_y * cells,
        [VMEM((planes, 3, rows_y, cells), jnp.float32)] * 2 + [pltpu.SemaphoreType.DMA((6 * planes,))],
        pltpu.HBM,
        limit=50 << 20,
        kind=jnp.bfloat16,
    )(velocity, vorticity)
    pieces = [(p, c) for p in range(planes) for c in range(3)]
    groups = (pieces[:EARLY], pieces[EARLY:])
    keeps, gots = [], []
    for group in groups:
        held = sorted({p for p, _ in group})
        spans = []
        for p in held:
            parts = [c for q, c in group if q == p]
            spans.append((parts[0] * rows_y, (parts[-1] + 1) * rows_y))
        n = len(group) * rows_y
        run = call(functools.partial(x_kernel, spans), [(n, keep)] * 2, 12 * n * cells * keep)
        mine, other = run(*[crosses[p] for p in held], table_x)
        keeps.append(mine)
        gots.append(lax.ppermute(other, "slab", [(0, 1), (1, 0)]))
    flops = 2 * 2 * keep * 3 * rows_y * keep
    kinds = EARLY * 4
    sent = call(
        functools.partial(y_send_kernel, rows_y),
        [(kinds * NXY, lanes)] * NZ,
        flops * EARLY,
        [VMEM((kinds * dests, lanes), jnp.float32)],
    )(keeps[0], gots[0], table_y)
    arrived = [sent[0]]
    for s in range(1, NZ):
        arrived.append(from_shift(sent[s], 0, s, 0))
    per = len(groups[1]) * 4
    packed = call(
        functools.partial(y_pack_kernel, rows_y), [(dests * per, lanes)], flops * len(groups[1])
    )(keeps[1], gots[1], table_y, sent[0])
    late = lax.all_to_all(
        packed.reshape(dests, per // 4, 4, lanes), GROUP, 0, 0, axis_index_groups=[order.tolist()], tiled=True
    )
    turned = call(turn_kernel, [(NZ * kinds, lanes)] * NXY, 0, [VMEM((NZ * kinds * NXY, lanes), jnp.float32)])(*arrived)
    spread = [turned[0]] + [from_shift(turned[d], d // NX, 0, d % NX) for d in range(1, NXY)]
    early_units = [[groups[0].index((p, c)) for p in range(planes) if (p, c) in groups[0]] for c in range(3)]
    late_units = [[groups[1].index((p, c)) for p in reversed(range(planes)) if (p, c) in groups[1]] for c in range(3)]
    most = [max(len(u) for u in units) for units in (early_units, late_units)]
    xy = xy_major_groups()[: dests // 2]
    near = order.reshape(NZ, 2, -1)[:, 0].reshape(-1)
    early_table = folded_z_table(cells, keep, np.concatenate([planes * xy + p for p in range(most[0])]))
    late_table = folded_z_table(
        cells, keep, np.concatenate([planes * near + planes - 1 - p for p in range(most[1])])
    )
    sums = VMEM((2, 2, 3, 2, keep // 2, lanes), jnp.float32)
    result = VMEM((3 * keep * 4, lanes), jnp.float32)
    early = call(
        functools.partial(early_kernel, keep, early_units),
        [(3 * keep * 4, lanes)],
        4 * EARLY * keep * 3 * dests * keep,
        [VMEM((kinds * dests, lanes), jnp.float32), sums, result, pltpu.SemaphoreType.DMA],
        [VMEM] * NXY + [pltpu.HBM, VMEM],
        limit=50 << 20,
    )(*spread, velocity_modes.reshape(3 * keep * 4, lanes), jnp.asarray(early_table))
    out = call(
        functools.partial(z_kernel, keep, late_units),
        [(3 * keep * 4, lanes)],
        4 * len(groups[1]) * keep * 3 * dests * keep,
        [sums, result, pltpu.SemaphoreType.DMA((6,))],
        out_space=pltpu.HBM,
    )(late.reshape(dests * per, lanes), early, jnp.asarray(late_table))
    return out.reshape(3, keep, rows_ky, 2, lanes)


def solution(mesh):
    return jax.shard_map(
        per_device,
        mesh=mesh,
        in_specs=(
            P(None, GROUP, "slab", None),
            P(None, GROUP, "slab", None),
            P(None, None, GROUP, None, "slab"),
        ),
        out_specs=P(None, None, GROUP, None, "slab"),
        check_vma=False,
    )
```

```python
import functools
import math

import jax
import jax.numpy as jnp
import ml_dtypes
import numpy as np
from jax import lax
from jax.experimental import pallas as pl
from jax.experimental.pallas import tpu as pltpu
from jax.sharding import PartitionSpec as P

VMEM = pltpu.VMEM
GROUP = ("section", "pen")
NY, NZ, NX = 4, 8, 4
NXY = NX * NY


def signed(index, count):
    return np.where(index < count // 2, index, index - count)


def halves(table):
    high = table.astype(np.float32).astype(ml_dtypes.bfloat16)
    low = (table - high.astype(np.float64)).astype(np.float32).astype(ml_dtypes.bfloat16)
    return high, low


def angles(modes, positions, length):
    return 2.0 * math.pi / length * ((modes[:, None] * positions[None, :]) % length)


def rows_of(theta, cells):
    return np.stack(halves(np.concatenate([np.cos(theta), np.sin(theta)], axis=0) / math.sqrt(cells)))


def z_major_groups():
    return np.array([(y * NZ + z) * NX + x for z in range(NZ) for y in range(NY) for x in range(NX)])


def xy_major_groups():
    return np.array([(y * NZ + z) * NX + x for y in range(NY) for x in range(NX) for z in range(NZ)])


def x_table(cells, keep):
    theta = angles(signed(np.arange(keep), keep), np.arange(cells), cells).T
    block = keep // 2
    parts = []
    for h in range(2):
        cut = theta[:, h * block : (h + 1) * block]
        parts += [np.cos(cut), -np.sin(cut)]
    return np.concatenate(halves(np.concatenate(parts, axis=1) / math.sqrt(cells)), axis=0)


def y_table(cells, keep, order):
    modes = signed(np.arange(keep), keep)
    return np.stack(
        [rows_of(angles(modes[parity::2][order], np.arange(cells // 2), cells), cells) for parity in range(2)]
    )


def folded_z_table(cells, keep, positions):
    modes = signed(np.arange(keep), keep)
    return np.stack([rows_of(angles(modes[parity::2], positions, cells), cells) for parity in range(2)])


def z_table(cells, keep, positions):
    return rows_of(angles(signed(np.arange(keep), keep), positions, cells), cells)


def split(x):
    high = x.astype(jnp.bfloat16)
    low = (x - high.astype(jnp.float32)).astype(jnp.bfloat16)
    return high, low


def product(a, b):
    return jnp.dot(a, b, preferred_element_type=jnp.float32)


def transformed(high_table, low_table, x):
    high, low = split(x)
    return product(
        jnp.concatenate([high_table, high_table, low_table], axis=1), jnp.concatenate([high, low, high], axis=0)
    )


def place():
    pen = lax.axis_index("pen")
    x = lax.rem(pen, NX)
    z = lax.rem(lax.div(pen, NX), NZ)
    y = lax.axis_index("section") * 2 + lax.div(pen, NX * NZ)
    return y, z, x


def cross_kernel(v_hbm, w_hbm, *refs):
    outs, (v_ref, w_ref, sems) = refs[:-3], refs[-3:]
    rows, cells = v_ref.shape[2:]
    copies = [
        [
            copy
            for c in range(3)
            for copy in (
                pltpu.make_async_copy(v_hbm.at[c, plane], v_ref.at[plane, c], sems.at[plane * 6 + c]),
                pltpu.make_async_copy(w_hbm.at[c, plane], w_ref.at[plane, c], sems.at[plane * 6 + 3 + c]),
            )
        ]
        for plane in range(len(outs))
    ]
    for group in copies:
        for copy in group:
            copy.start()
    for plane, out_ref in enumerate(outs):
        for copy in copies[plane]:
            copy.wait()
        for c in range(3):
            a, b = (c + 1) % 3, (c + 2) % 3
            high, low = split(v_ref[plane, a] * w_ref[plane, b] - v_ref[plane, b] * w_ref[plane, a])
            out_ref[c * rows : (c + 1) * rows, :cells] = high
            out_ref[c * rows : (c + 1) * rows, cells:] = low


def x_kernel(*refs):
    planes, (table_ref, keep_ref, send_ref) = refs[:-3], refs[-3:]
    cells = planes[0].shape[1] // 2
    rows = planes[0].shape[0]
    half = keep_ref.shape[-1]
    mine = lax.axis_index("slab") == 0
    table = jnp.concatenate([table_ref[:cells], table_ref[:cells], table_ref[cells:]], axis=0)
    for i, ref in enumerate(planes):
        both = ref[...]
        out = product(jnp.concatenate([both, both[:, :cells]], axis=1), table)
        first, second = out[:, :half], out[:, half:]
        here = slice(i * rows, (i + 1) * rows)
        keep_ref[here] = jnp.where(mine, first, second)
        send_ref[here] = jnp.where(mine, second, first)


def y_blocks(keep_ref, got_ref, table_ref, rows):
    sign = jnp.where(lax.axis_index("slab") == 0, 1.0, -1.0).astype(jnp.float32)
    dests = table_ref.shape[2] // 2
    lanes = keep_ref.shape[1] // 2
    for block in range(keep_ref.shape[0] // rows):
        here = slice(block * rows, (block + 1) * rows)
        own, got = keep_ref[here], got_ref[here]
        for parity in range(2):
            folded = own + got if parity == 0 else (own - got) * sign
            out = transformed(table_ref[parity, 0], table_ref[parity, 1], folded)
            yield block, parity * 2, out[:dests, :lanes] + out[dests:, lanes:]
            yield block, parity * 2 + 1, out[:dests, lanes:] - out[dests:, :lanes]


def y_pack_kernel(rows, keep_ref, got_ref, table_ref, _, out_ref):
    dests = table_ref.shape[2] // 2
    per = out_ref.shape[0] // dests
    for block, q, value in y_blocks(keep_ref, got_ref, table_ref, rows):
        out_ref[pl.ds(block * 4 + q, dests, per), :] = value


def y_send_kernel(rows, keep_ref, got_ref, table_ref, *refs):
    outs, all_ref = refs[:-1], refs[-1]
    dests = table_ref.shape[2] // 2
    for block, q, value in y_blocks(keep_ref, got_ref, table_ref, rows):
        at = (block * 4 + q) * dests
        all_ref[at : at + dests] = value
    _, z, _ = place()
    for shift in range(NZ):
        to = lax.rem(z - shift + NZ, NZ)
        for k in range(all_ref.shape[0] // dests):
            outs[shift][k * NXY : (k + 1) * NXY] = all_ref[pl.ds(pl.multiple_of(k * dests + to * NXY, NXY), NXY), :]


def turn_kernel(*refs):
    gots, outs, all_ref = refs[:NZ], refs[NZ:-1], refs[-1]
    y, z, x = place()
    size = gots[0].shape[0]
    for shift in range(NZ):
        source = lax.rem(z + shift, NZ)
        all_ref[pl.ds(pl.multiple_of(source * size, size), size), :] = gots[shift][...]
    count = all_ref.shape[0] // NXY
    for dy in range(NY):
        for dx in range(NX):
            to = lax.rem(y - dy + NY, NY) * NX + lax.rem(x - dx + NX, NX)
            outs[dy * NX + dx][...] = all_ref[pl.ds(to, count, NXY), :]


def wave_numbers(keep, lanes, first, count, step):
    group = lax.axis_index("section") * lax.axis_size("pen") + lax.axis_index("pen")
    limit = -(keep // 2)
    visc = 0.5 / (keep // 2) ** 2
    row = lax.broadcasted_iota(jnp.int32, (count, lanes), 0) * step + first
    col = lax.broadcasted_iota(jnp.int32, (count, lanes), 1) + lax.axis_index("slab") * lanes
    kz = jnp.where(row < keep // 2, row, row - keep)
    kx = jnp.where(col < keep // 2, col, col - keep)
    for parity in range(2):
        index = group * 2 + parity
        ky = jnp.where(index < keep // 2, index, index - keep)
        mask = ((kx != limit) & (kz != limit) & (ky != limit)).astype(jnp.float32)
        waves = (kx.astype(jnp.float32), ky.astype(jnp.float32), kz.astype(jnp.float32))
        ksq = waves[0] * waves[0] + waves[1] * waves[1] + waves[2] * waves[2]
        yield parity, waves, mask, 1.0 / jnp.maximum(ksq, 1.0), visc * ksq


def projected(s, waves, mask, inverse):
    inner = (waves[0] * s[0] + waves[1] * s[1] + waves[2] * s[2]) * inverse
    return [mask * (s[c] - waves[c] * inner) for c in range(3)]


def z_sums(keep, lanes, table, columns):
    out = transformed(table[0], table[1], columns)
    return out[:keep, :lanes] + out[keep:, lanes:], out[:keep, lanes:] - out[keep:, :lanes]


def early_kernel(keep, *refs):
    gots, (modes_hbm, table_ref, out_ref, all_ref, modes_ref, sems) = refs[:NXY], refs[NXY:]
    copies = []
    part = modes_ref.shape[0] // sems.shape[0]
    for i in range(sems.shape[0]):
        rows = pl.ds(i * part, part)
        copies.append(pltpu.make_async_copy(modes_hbm.at[rows], modes_ref.at[rows], sems.at[i]))
        copies[-1].start()
    y, _, x = place()
    lanes = out_ref.shape[1]
    kinds = gots[0].shape[0] // NZ
    sources = NXY * NZ
    for dy in range(NY):
        for dx in range(NX):
            source = lax.rem(y + dy, NY) * NX + lax.rem(x + dx, NX)
            for k in range(kinds):
                at = pl.multiple_of(k * sources + source * NZ, NZ)
                all_ref[pl.ds(at, NZ), :] = gots[dy * NX + dx][pl.ds(k, NZ, kinds), :]
    sums = []
    for parity in range(2):
        for c in range(3):
            base = c * 4 + parity * 2
            both = [all_ref[(base + q) * sources : (base + q + 1) * sources] for q in range(2)]
            sums.append(z_sums(keep, lanes, table_ref, jnp.concatenate(both, axis=1)))
    for copy in copies:
        copy.wait()
    for parity, waves, mask, inverse, damp in wave_numbers(keep, lanes, 0, keep, 1):
        for q in range(2):
            s = [sums[parity * 3 + c][q] for c in range(3)]
            for c, value in enumerate(projected(s, waves, mask, inverse)):
                where = pl.ds(c * keep * 4 + parity * 2 + q, keep, 4)
                at = ((c * 2 + parity) * 2 + q) * keep
                out_ref[at : at + keep] = value - damp * modes_ref[where, :]


def z_kernel(planes, keep, x_ref, early_ref, table_ref, out_hbm, sums_ref, out_ref, sems):
    lanes = x_ref.shape[1]
    per = 3 * planes * 4
    sources = x_ref.shape[0] // per
    run = NXY // 2
    for parity in range(2):
        for c in range(3):
            sums, differences = [], []
            for p in range(planes):
                at = (p * 3 + c) * 4 + parity * 2
                both = jnp.concatenate([x_ref[pl.ds(at + q, sources, per), :] for q in range(2)], axis=1)
                both = both.reshape(NZ, 2, run, 2 * lanes)
                sums.append((both[:, 0] + both[:, 1]).reshape(NZ * run, 2 * lanes))
                differences.append((both[:, 0] - both[:, 1]).reshape(NZ * run, 2 * lanes))
            for e, folded in enumerate((sums, differences)):
                pair = z_sums(keep // 2, lanes, table_ref.at[e], jnp.concatenate(folded, axis=0))
                for q in range(2):
                    sums_ref[parity, q, c, e] = pair[q]
    count = sems.shape[0] // 3
    part = keep // 2 // count
    copies = []
    for h in range(count):
        here = slice(h * part, (h + 1) * part)
        for e in range(2):
            for parity, waves, mask, inverse, _ in wave_numbers(keep, lanes, h * part * 2 + e, part, 2):
                for q in range(2):
                    values = projected([sums_ref[parity, q, c, e, here] for c in range(3)], waves, mask, inverse)
                    for c, value in enumerate(values):
                        where = pl.ds((c * keep + h * part * 2 + e) * 4 + parity * 2 + q, part, 8)
                        at = ((c * 2 + parity) * 2 + q) * keep + h * part * 2 + e
                        out_ref[where, :] = value + early_ref[pl.ds(at, part, 2), :]
        for c in range(3):
            rows = pl.ds((c * keep + h * part * 2) * 4, part * 8)
            copies.append(pltpu.make_async_copy(out_ref.at[rows], out_hbm.at[rows], sems.at[h * 3 + c]))
            copies[-1].start()
    for copy in copies:
        copy.wait()


def call(kernel, outs, flops=0, scratch=(), space=VMEM, out_space=VMEM, limit=40 << 20, kind=jnp.float32):
    def run(*args):
        size = sum(a.size * a.dtype.itemsize for a in args) + sum(4 * math.prod(o) for o in outs)
        shapes = [jax.ShapeDtypeStruct(o, kind) for o in outs]
        specs = [pl.BlockSpec(memory_space=out_space)] * len(outs)
        single = len(outs) == 1
        return pl.pallas_call(
            kernel,
            out_shape=shapes[0] if single else shapes,
            in_specs=[pl.BlockSpec(memory_space=m) for m in (space if isinstance(space, list) else [space] * len(args))],
            out_specs=specs[0] if single else specs,
            scratch_shapes=list(scratch),
            cost_estimate=pl.CostEstimate(flops=flops, bytes_accessed=size, transcendentals=0),
            compiler_params=pltpu.CompilerParams(vmem_limit_bytes=limit),
        )(*args)

    return run


def group_of(y, z, x):
    return ((y % NY) * NZ + z % NZ) * NX + x % NX


def from_shift(value, dy, dz, dx):
    pairs = [
        (group_of(y + dy, z + dz, x + dx), group_of(y, z, x))
        for y in range(NY)
        for z in range(NZ)
        for x in range(NX)
    ]
    return lax.ppermute(value, GROUP, pairs)


def per_device(velocity, vorticity, velocity_modes):
    _, planes, rows_y, cells = velocity.shape
    _, keep, rows_ky, _, lanes = velocity_modes.shape
    dests = lax.axis_size(GROUP)
    order = z_major_groups()
    table_y = jnp.asarray(y_table(cells, keep, order))
    table_x = jnp.asarray(x_table(cells, keep))
    crosses = call(
        cross_kernel,
        [(3 * rows_y, 2 * cells)] * planes,
        6 * planes * 3 * rows_y * cells,
        [VMEM((planes, 3, rows_y, cells), jnp.float32)] * 2 + [pltpu.SemaphoreType.DMA((6 * planes,))],
        pltpu.HBM,
        limit=50 << 20,
        kind=jnp.bfloat16,
    )(velocity, vorticity)
    keeps, gots = [], []
    for held in (crosses[:1], crosses[1:]):
        n = len(held)
        run = call(x_kernel, [(3 * n * rows_y, keep)] * 2, 2 * 9 * n * rows_y * cells * 2 * keep)
        mine, other = run(*held, table_x)
        keeps.append(mine)
        gots.append(lax.ppermute(other, "slab", [(0, 1), (1, 0)]))
    flops = 2 * 3 * 2 * keep * 3 * rows_y * keep
    kinds = 3 * 4
    sent = call(
        functools.partial(y_send_kernel, rows_y),
        [(kinds * NXY, lanes)] * NZ,
        flops,
        [VMEM((kinds * dests, lanes), jnp.float32)],
    )(keeps[0], gots[0], table_y)
    arrived = [sent[0]]
    for s in range(1, NZ):
        arrived.append(from_shift(sent[s], 0, s, 0))
    per = (planes - 1) * kinds
    packed = call(
        functools.partial(y_pack_kernel, rows_y), [(dests * per, lanes)], flops * (planes - 1)
    )(keeps[1], gots[1], table_y, sent[0])
    late = lax.all_to_all(
        packed.reshape(dests, per, lanes), GROUP, 0, 0, axis_index_groups=[order.tolist()], tiled=True
    )
    turned = call(turn_kernel, [(NZ * kinds, lanes)] * NXY, 0, [VMEM((NZ * kinds * NXY, lanes), jnp.float32)])(*arrived)
    spread = [turned[0]] + [from_shift(turned[d], d // NX, 0, d % NX) for d in range(1, NXY)]
    early = call(
        functools.partial(early_kernel, keep),
        [(3 * keep * 4, lanes)],
        2 * 6 * 2 * keep * 3 * dests * keep,
        [
            VMEM((kinds * dests, lanes), jnp.float32),
            VMEM((3 * keep * 4, lanes), jnp.float32),
            pltpu.SemaphoreType.DMA((6,)),
        ],
        [VMEM] * NXY + [pltpu.HBM, VMEM],
        limit=50 << 20,
    )(
        *spread,
        velocity_modes.reshape(3 * keep * 4, lanes),
        jnp.asarray(z_table(cells, keep, planes * xy_major_groups())),
    )
    near = order.reshape(NZ, 2, -1)[:, 0].reshape(-1)
    rest = np.concatenate([planes * near + p for p in range(1, planes)])
    table_z = jnp.asarray(folded_z_table(cells, keep, rest))
    out = call(
        functools.partial(z_kernel, planes - 1, keep),
        [(3 * keep * 4, lanes)],
        6 * 2 * keep * 3 * (planes - 1) * dests * keep,
        [
            VMEM((2, 2, 3, 2, keep // 2, lanes), jnp.float32),
            VMEM((3 * keep * 4, lanes), jnp.float32),
            pltpu.SemaphoreType.DMA((6,)),
        ],
        out_space=pltpu.HBM,
    )(late.reshape(dests * per, lanes), early, table_z)
    return out.reshape(3, keep, rows_ky, 2, lanes)


def solution(mesh):
    return jax.shard_map(
        per_device,
        mesh=mesh,
        in_specs=(
            P(None, GROUP, "slab", None),
            P(None, GROUP, "slab", None),
            P(None, None, GROUP, None, "slab"),
        ),
        out_specs=P(None, None, GROUP, None, "slab"),
        check_vma=False,
    )
```

```python
import functools
import math

import jax
import jax.numpy as jnp
import ml_dtypes
import numpy as np
from jax import lax
from jax.experimental import pallas as pl
from jax.experimental.pallas import tpu as pltpu
from jax.sharding import PartitionSpec as P

VMEM = pltpu.VMEM
GROUP = ("section", "pen")
NY, NZ, NX = 4, 8, 4
NXY = NX * NY


def signed(index, count):
    return np.where(index < count // 2, index, index - count)


def halves(table):
    high = table.astype(np.float32).astype(ml_dtypes.bfloat16)
    low = (table - high.astype(np.float64)).astype(np.float32).astype(ml_dtypes.bfloat16)
    return high, low


def angles(modes, positions, length):
    return 2.0 * math.pi / length * ((modes[:, None] * positions[None, :]) % length)


def rows_of(theta, cells):
    return np.stack(halves(np.concatenate([np.cos(theta), np.sin(theta)], axis=0) / math.sqrt(cells)))


def z_major_groups():
    return np.array([(y * NZ + z) * NX + x for z in range(NZ) for y in range(NY) for x in range(NX)])


def xy_major_groups():
    return np.array([(y * NZ + z) * NX + x for y in range(NY) for x in range(NX) for z in range(NZ)])


def x_table(cells, keep):
    theta = angles(signed(np.arange(keep), keep), np.arange(cells), cells).T
    block = keep // 2
    parts = []
    for h in range(2):
        cut = theta[:, h * block : (h + 1) * block]
        parts += [np.cos(cut), -np.sin(cut)]
    return np.concatenate(halves(np.concatenate(parts, axis=1) / math.sqrt(cells)), axis=0)


def y_table(cells, keep, order):
    modes = signed(np.arange(keep), keep)
    return np.stack(
        [rows_of(angles(modes[parity::2][order], np.arange(cells // 2), cells), cells) for parity in range(2)]
    )


def folded_z_table(cells, keep, positions):
    modes = signed(np.arange(keep), keep)
    return np.stack([rows_of(angles(modes[parity::2], positions, cells), cells) for parity in range(2)])


def z_table(cells, keep, positions):
    return rows_of(angles(signed(np.arange(keep), keep), positions, cells), cells)


def split(x):
    high = x.astype(jnp.bfloat16)
    low = (x - high.astype(jnp.float32)).astype(jnp.bfloat16)
    return high, low


def product(a, b):
    return jnp.dot(a, b, preferred_element_type=jnp.float32)


def transformed(high_table, low_table, x):
    high, low = split(x)
    return product(
        jnp.concatenate([high_table, high_table, low_table], axis=1), jnp.concatenate([high, low, high], axis=0)
    )


def place():
    pen = lax.axis_index("pen")
    x = lax.rem(pen, NX)
    z = lax.rem(lax.div(pen, NX), NZ)
    y = lax.axis_index("section") * 2 + lax.div(pen, NX * NZ)
    return y, z, x


def cross_kernel(v_hbm, w_hbm, *refs):
    outs, (v_ref, w_ref, sems) = refs[:-3], refs[-3:]
    rows, cells = v_ref.shape[2:]
    copies = [
        [
            copy
            for c in range(3)
            for copy in (
                pltpu.make_async_copy(v_hbm.at[c, plane], v_ref.at[plane, c], sems.at[plane * 6 + c]),
                pltpu.make_async_copy(w_hbm.at[c, plane], w_ref.at[plane, c], sems.at[plane * 6 + 3 + c]),
            )
        ]
        for plane in range(len(outs))
    ]
    for group in copies[:2]:
        for copy in group:
            copy.start()
    for plane, out_ref in enumerate(outs):
        for copy in copies[plane]:
            copy.wait()
        for group in copies[plane + 2 : plane + 3]:
            for copy in group:
                copy.start()
        for c in range(3):
            a, b = (c + 1) % 3, (c + 2) % 3
            high, low = split(v_ref[plane, a] * w_ref[plane, b] - v_ref[plane, b] * w_ref[plane, a])
            out_ref[c * rows : (c + 1) * rows, :cells] = high
            out_ref[c * rows : (c + 1) * rows, cells:] = low


def x_kernel(*refs):
    planes, (table_ref, keep_ref, send_ref) = refs[:-3], refs[-3:]
    cells = planes[0].shape[1] // 2
    rows = planes[0].shape[0]
    half = keep_ref.shape[-1]
    mine = lax.axis_index("slab") == 0
    table = jnp.concatenate([table_ref[:cells], table_ref[:cells], table_ref[cells:]], axis=0)
    for i, ref in enumerate(planes):
        both = ref[...]
        out = product(jnp.concatenate([both, both[:, :cells]], axis=1), table)
        first, second = out[:, :half], out[:, half:]
        here = slice(i * rows, (i + 1) * rows)
        keep_ref[here] = jnp.where(mine, first, second)
        send_ref[here] = jnp.where(mine, second, first)


def y_blocks(keep_ref, got_ref, table_ref, rows):
    sign = jnp.where(lax.axis_index("slab") == 0, 1.0, -1.0).astype(jnp.float32)
    dests = table_ref.shape[2] // 2
    lanes = keep_ref.shape[1] // 2
    for block in range(keep_ref.shape[0] // rows):
        here = slice(block * rows, (block + 1) * rows)
        own, got = keep_ref[here], got_ref[here]
        for parity in range(2):
            folded = own + got if parity == 0 else (own - got) * sign
            out = transformed(table_ref[parity, 0], table_ref[parity, 1], folded)
            yield block, parity * 2, out[:dests, :lanes] + out[dests:, lanes:]
            yield block, parity * 2 + 1, out[:dests, lanes:] - out[dests:, :lanes]


def y_pack_kernel(rows, keep_ref, got_ref, table_ref, _, out_ref):
    dests = table_ref.shape[2] // 2
    per = out_ref.shape[0] // dests
    for block, q, value in y_blocks(keep_ref, got_ref, table_ref, rows):
        out_ref[pl.ds(block * 4 + q, dests, per), :] = value


def y_send_kernel(rows, keep_ref, got_ref, table_ref, *refs):
    outs, all_ref = refs[:-1], refs[-1]
    dests = table_ref.shape[2] // 2
    for block, q, value in y_blocks(keep_ref, got_ref, table_ref, rows):
        at = (block * 4 + q) * dests
        all_ref[at : at + dests] = value
    _, z, _ = place()
    for shift in range(NZ):
        to = lax.rem(z - shift + NZ, NZ)
        for k in range(all_ref.shape[0] // dests):
            outs[shift][k * NXY : (k + 1) * NXY] = all_ref[pl.ds(pl.multiple_of(k * dests + to * NXY, NXY), NXY), :]


def turn_kernel(*refs):
    gots, outs, all_ref = refs[:NZ], refs[NZ:-1], refs[-1]
    y, z, x = place()
    size = gots[0].shape[0]
    for shift in range(NZ):
        source = lax.rem(z + shift, NZ)
        all_ref[pl.ds(pl.multiple_of(source * size, size), size), :] = gots[shift][...]
    count = all_ref.shape[0] // NXY
    for dy in range(NY):
        for dx in range(NX):
            to = lax.rem(y - dy + NY, NY) * NX + lax.rem(x - dx + NX, NX)
            outs[dy * NX + dx][...] = all_ref[pl.ds(to, count, NXY), :]


def wave_numbers(keep, lanes, first, count, step):
    group = lax.axis_index("section") * lax.axis_size("pen") + lax.axis_index("pen")
    limit = -(keep // 2)
    visc = 0.5 / (keep // 2) ** 2
    row = lax.broadcasted_iota(jnp.int32, (count, lanes), 0) * step + first
    col = lax.broadcasted_iota(jnp.int32, (count, lanes), 1) + lax.axis_index("slab") * lanes
    kz = jnp.where(row < keep // 2, row, row - keep)
    kx = jnp.where(col < keep // 2, col, col - keep)
    for parity in range(2):
        index = group * 2 + parity
        ky = jnp.where(index < keep // 2, index, index - keep)
        mask = ((kx != limit) & (kz != limit) & (ky != limit)).astype(jnp.float32)
        waves = (kx.astype(jnp.float32), ky.astype(jnp.float32), kz.astype(jnp.float32))
        ksq = waves[0] * waves[0] + waves[1] * waves[1] + waves[2] * waves[2]
        yield parity, waves, mask, 1.0 / jnp.maximum(ksq, 1.0), visc * ksq


def projected(s, waves, mask, inverse):
    inner = (waves[0] * s[0] + waves[1] * s[1] + waves[2] * s[2]) * inverse
    return [mask * (s[c] - waves[c] * inner) for c in range(3)]


def z_sums(keep, lanes, table, columns):
    out = transformed(table[0], table[1], columns)
    return out[:keep, :lanes] + out[keep:, lanes:], out[:keep, lanes:] - out[keep:, :lanes]


def early_kernel(keep, *refs):
    gots, (modes_hbm, table_ref, out_ref, all_ref, modes_ref, sems) = refs[:NXY], refs[NXY:]
    copies = []
    part = modes_ref.shape[0] // sems.shape[0]
    for i in range(sems.shape[0]):
        rows = pl.ds(i * part, part)
        copies.append(pltpu.make_async_copy(modes_hbm.at[rows], modes_ref.at[rows], sems.at[i]))
        copies[-1].start()
    y, _, x = place()
    lanes = out_ref.shape[1]
    kinds = gots[0].shape[0] // NZ
    sources = NXY * NZ
    for dy in range(NY):
        for dx in range(NX):
            source = lax.rem(y + dy, NY) * NX + lax.rem(x + dx, NX)
            for k in range(kinds):
                at = pl.multiple_of(k * sources + source * NZ, NZ)
                all_ref[pl.ds(at, NZ), :] = gots[dy * NX + dx][pl.ds(k, NZ, kinds), :]
    sums = []
    for parity in range(2):
        for c in range(3):
            base = c * 4 + parity * 2
            both = [all_ref[(base + q) * sources : (base + q + 1) * sources] for q in range(2)]
            sums.append(z_sums(keep, lanes, table_ref, jnp.concatenate(both, axis=1)))
    for copy in copies:
        copy.wait()
    for parity, waves, mask, inverse, damp in wave_numbers(keep, lanes, 0, keep, 1):
        for q in range(2):
            s = [sums[parity * 3 + c][q] for c in range(3)]
            for c, value in enumerate(projected(s, waves, mask, inverse)):
                where = pl.ds(c * keep * 4 + parity * 2 + q, keep, 4)
                at = ((c * 2 + parity) * 2 + q) * keep
                out_ref[at : at + keep] = value - damp * modes_ref[where, :]


def z_kernel(planes, keep, x_ref, early_ref, table_ref, out_hbm, sums_ref, out_ref, sems):
    lanes = x_ref.shape[1]
    per = 3 * planes * 4
    sources = x_ref.shape[0] // per
    run = NXY // 2
    for parity in range(2):
        for c in range(3):
            sums, differences = [], []
            for p in range(planes):
                at = (p * 3 + c) * 4 + parity * 2
                both = jnp.concatenate([x_ref[pl.ds(at + q, sources, per), :] for q in range(2)], axis=1)
                both = both.reshape(NZ, 2, run, 2 * lanes)
                sums.append((both[:, 0] + both[:, 1]).reshape(NZ * run, 2 * lanes))
                differences.append((both[:, 0] - both[:, 1]).reshape(NZ * run, 2 * lanes))
            for e, folded in enumerate((sums, differences)):
                pair = z_sums(keep // 2, lanes, table_ref.at[e], jnp.concatenate(folded, axis=0))
                for q in range(2):
                    sums_ref[parity, q, c, e] = pair[q]
    count = sems.shape[0] // 3
    part = keep // 2 // count
    copies = []
    for h in range(count):
        here = slice(h * part, (h + 1) * part)
        for e in range(2):
            for parity, waves, mask, inverse, _ in wave_numbers(keep, lanes, h * part * 2 + e, part, 2):
                for q in range(2):
                    values = projected([sums_ref[parity, q, c, e, here] for c in range(3)], waves, mask, inverse)
                    for c, value in enumerate(values):
                        where = pl.ds((c * keep + h * part * 2 + e) * 4 + parity * 2 + q, part, 8)
                        at = ((c * 2 + parity) * 2 + q) * keep + h * part * 2 + e
                        out_ref[where, :] = value + early_ref[pl.ds(at, part, 2), :]
        for c in range(3):
            rows = pl.ds((c * keep + h * part * 2) * 4, part * 8)
            copies.append(pltpu.make_async_copy(out_ref.at[rows], out_hbm.at[rows], sems.at[h * 3 + c]))
            copies[-1].start()
    for copy in copies:
        copy.wait()


def call(kernel, outs, flops=0, scratch=(), space=VMEM, out_space=VMEM, limit=40 << 20, kind=jnp.float32):
    def run(*args):
        size = sum(a.size * a.dtype.itemsize for a in args) + sum(4 * math.prod(o) for o in outs)
        shapes = [jax.ShapeDtypeStruct(o, kind) for o in outs]
        specs = [pl.BlockSpec(memory_space=out_space)] * len(outs)
        single = len(outs) == 1
        return pl.pallas_call(
            kernel,
            out_shape=shapes[0] if single else shapes,
            in_specs=[pl.BlockSpec(memory_space=m) for m in (space if isinstance(space, list) else [space] * len(args))],
            out_specs=specs[0] if single else specs,
            scratch_shapes=list(scratch),
            cost_estimate=pl.CostEstimate(flops=flops, bytes_accessed=size, transcendentals=0),
            compiler_params=pltpu.CompilerParams(vmem_limit_bytes=limit),
        )(*args)

    return run


def group_of(y, z, x):
    return ((y % NY) * NZ + z % NZ) * NX + x % NX


def from_shift(value, dy, dz, dx):
    pairs = [
        (group_of(y + dy, z + dz, x + dx), group_of(y, z, x))
        for y in range(NY)
        for z in range(NZ)
        for x in range(NX)
    ]
    return lax.ppermute(value, GROUP, pairs)


def per_device(velocity, vorticity, velocity_modes):
    _, planes, rows_y, cells = velocity.shape
    _, keep, rows_ky, _, lanes = velocity_modes.shape
    dests = lax.axis_size(GROUP)
    order = z_major_groups()
    table_y = jnp.asarray(y_table(cells, keep, order))
    table_x = jnp.asarray(x_table(cells, keep))
    crosses = call(
        cross_kernel,
        [(3 * rows_y, 2 * cells)] * planes,
        6 * planes * 3 * rows_y * cells,
        [VMEM((planes, 3, rows_y, cells), jnp.float32)] * 2 + [pltpu.SemaphoreType.DMA((6 * planes,))],
        pltpu.HBM,
        limit=50 << 20,
        kind=jnp.bfloat16,
    )(velocity, vorticity)
    keeps, gots = [], []
    for held in (crosses[:1], crosses[1:]):
        n = len(held)
        run = call(x_kernel, [(3 * n * rows_y, keep)] * 2, 2 * 9 * n * rows_y * cells * 2 * keep)
        mine, other = run(*held, table_x)
        keeps.append(mine)
        gots.append(lax.ppermute(other, "slab", [(0, 1), (1, 0)]))
    flops = 2 * 3 * 2 * keep * 3 * rows_y * keep
    kinds = 3 * 4
    sent = call(
        functools.partial(y_send_kernel, rows_y),
        [(kinds * NXY, lanes)] * NZ,
        flops,
        [VMEM((kinds * dests, lanes), jnp.float32)],
    )(keeps[0], gots[0], table_y)
    arrived = [sent[0]]
    for s in range(1, NZ):
        arrived.append(from_shift(sent[s], 0, s, 0))
    per = (planes - 1) * kinds
    packed = call(
        functools.partial(y_pack_kernel, rows_y), [(dests * per, lanes)], flops * (planes - 1)
    )(keeps[1], gots[1], table_y, sent[0])
    late = lax.all_to_all(
        packed.reshape(dests, per, lanes), GROUP, 0, 0, axis_index_groups=[order.tolist()], tiled=True
    )
    turned = call(turn_kernel, [(NZ * kinds, lanes)] * NXY, 0, [VMEM((NZ * kinds * NXY, lanes), jnp.float32)])(*arrived)
    spread = [turned[0]] + [from_shift(turned[d], d // NX, 0, d % NX) for d in range(1, NXY)]
    early = call(
        functools.partial(early_kernel, keep),
        [(3 * keep * 4, lanes)],
        2 * 6 * 2 * keep * 3 * dests * keep,
        [
            VMEM((kinds * dests, lanes), jnp.float32),
            VMEM((3 * keep * 4, lanes), jnp.float32),
            pltpu.SemaphoreType.DMA((6,)),
        ],
        [VMEM] * NXY + [pltpu.HBM, VMEM],
        limit=50 << 20,
    )(
        *spread,
        velocity_modes.reshape(3 * keep * 4, lanes),
        jnp.asarray(z_table(cells, keep, planes * xy_major_groups())),
    )
    near = order.reshape(NZ, 2, -1)[:, 0].reshape(-1)
    rest = np.concatenate([planes * near + p for p in range(1, planes)])
    table_z = jnp.asarray(folded_z_table(cells, keep, rest))
    out = call(
        functools.partial(z_kernel, planes - 1, keep),
        [(3 * keep * 4, lanes)],
        6 * 2 * keep * 3 * (planes - 1) * dests * keep,
        [
            VMEM((2, 2, 3, 2, keep // 2, lanes), jnp.float32),
            VMEM((3 * keep * 4, lanes), jnp.float32),
            pltpu.SemaphoreType.DMA((6,)),
        ],
        out_space=pltpu.HBM,
    )(late.reshape(dests * per, lanes), early, table_z)
    return out.reshape(3, keep, rows_ky, 2, lanes)


def solution(mesh):
    return jax.shard_map(
        per_device,
        mesh=mesh,
        in_specs=(
            P(None, GROUP, "slab", None),
            P(None, GROUP, "slab", None),
            P(None, None, GROUP, None, "slab"),
        ),
        out_specs=P(None, None, GROUP, None, "slab"),
        check_vma=False,
    )
```

```python
import functools
import math

import jax
import jax.numpy as jnp
import ml_dtypes
import numpy as np
from jax import lax
from jax.experimental import pallas as pl
from jax.experimental.pallas import tpu as pltpu
from jax.sharding import PartitionSpec as P

VMEM = pltpu.VMEM
GROUP = ("section", "pen")
NY, NZ, NX = 4, 8, 4
NXY = NX * NY


def signed(index, count):
    return np.where(index < count // 2, index, index - count)


def halves(table):
    high = table.astype(np.float32).astype(ml_dtypes.bfloat16)
    low = (table - high.astype(np.float64)).astype(np.float32).astype(ml_dtypes.bfloat16)
    return high, low


def angles(modes, positions, length):
    return 2.0 * math.pi / length * ((modes[:, None] * positions[None, :]) % length)


def rows_of(theta, cells):
    return np.stack(halves(np.concatenate([np.cos(theta), np.sin(theta)], axis=0) / math.sqrt(cells)))


def z_major_groups():
    return np.array([(y * NZ + z) * NX + x for z in range(NZ) for y in range(NY) for x in range(NX)])


def xy_major_groups():
    return np.array([(y * NZ + z) * NX + x for y in range(NY) for x in range(NX) for z in range(NZ)])


def x_table(cells, keep):
    theta = angles(signed(np.arange(keep), keep), np.arange(cells), cells).T
    block = keep // 2
    parts = []
    for h in range(2):
        cut = theta[:, h * block : (h + 1) * block]
        parts += [np.cos(cut), -np.sin(cut)]
    return np.concatenate(halves(np.concatenate(parts, axis=1) / math.sqrt(cells)), axis=0)


def y_table(cells, keep, order):
    modes = signed(np.arange(keep), keep)
    return np.stack(
        [rows_of(angles(modes[parity::2][order], np.arange(cells // 2), cells), cells) for parity in range(2)]
    )


def folded_z_table(cells, keep, positions):
    modes = signed(np.arange(keep), keep)
    return np.stack([rows_of(angles(modes[parity::2], positions, cells), cells) for parity in range(2)])


def z_table(cells, keep, positions):
    return rows_of(angles(signed(np.arange(keep), keep), positions, cells), cells)


def split(x):
    high = x.astype(jnp.bfloat16)
    low = (x - high.astype(jnp.float32)).astype(jnp.bfloat16)
    return high, low


def product(a, b):
    return jnp.dot(a, b, preferred_element_type=jnp.float32)


def transformed(high_table, low_table, x):
    high, low = split(x)
    return product(
        jnp.concatenate([high_table, high_table, low_table], axis=1), jnp.concatenate([high, low, high], axis=0)
    )


def place():
    pen = lax.axis_index("pen")
    x = lax.rem(pen, NX)
    z = lax.rem(lax.div(pen, NX), NZ)
    y = lax.axis_index("section") * 2 + lax.div(pen, NX * NZ)
    return y, z, x


def cross_kernel(v_hbm, w_hbm, *refs):
    outs, (v_ref, w_ref, sems) = refs[:-3], refs[-3:]
    rows, cells = v_ref.shape[2:]
    part = rows // 2
    copies = [
        [
            pltpu.make_async_copy(
                hbm.at[c, plane, pl.ds(i * part, part)],
                ref.at[plane, c, pl.ds(i * part, part)],
                sems.at[((plane * 3 + c) * 2 + i) * 2 + k],
            )
            for c in range(3)
            for i in range(2)
            for k, (hbm, ref) in enumerate(((v_hbm, v_ref), (w_hbm, w_ref)))
        ]
        for plane in range(len(outs))
    ]
    for group in copies:
        for copy in group:
            copy.start()
    for plane, out_ref in enumerate(outs):
        for copy in copies[plane]:
            copy.wait()
        for c in range(3):
            a, b = (c + 1) % 3, (c + 2) % 3
            high, low = split(v_ref[plane, a] * w_ref[plane, b] - v_ref[plane, b] * w_ref[plane, a])
            out_ref[c * rows : (c + 1) * rows, :cells] = high
            out_ref[c * rows : (c + 1) * rows, cells:] = low


def x_kernel(*refs):
    planes, (table_ref, keep_ref, send_ref) = refs[:-3], refs[-3:]
    cells = planes[0].shape[1] // 2
    rows = planes[0].shape[0]
    half = keep_ref.shape[-1]
    mine = lax.axis_index("slab") == 0
    table = jnp.concatenate([table_ref[:cells], table_ref[:cells], table_ref[cells:]], axis=0)
    for i, ref in enumerate(planes):
        both = ref[...]
        out = product(jnp.concatenate([both, both[:, :cells]], axis=1), table)
        first, second = out[:, :half], out[:, half:]
        here = slice(i * rows, (i + 1) * rows)
        keep_ref[here] = jnp.where(mine, first, second)
        send_ref[here] = jnp.where(mine, second, first)


def y_blocks(keep_ref, got_ref, table_ref, rows):
    sign = jnp.where(lax.axis_index("slab") == 0, 1.0, -1.0).astype(jnp.float32)
    dests = table_ref.shape[2] // 2
    lanes = keep_ref.shape[1] // 2
    for block in range(keep_ref.shape[0] // rows):
        here = slice(block * rows, (block + 1) * rows)
        own, got = keep_ref[here], got_ref[here]
        for parity in range(2):
            folded = own + got if parity == 0 else (own - got) * sign
            out = transformed(table_ref[parity, 0], table_ref[parity, 1], folded)
            yield block, parity * 2, out[:dests, :lanes] + out[dests:, lanes:]
            yield block, parity * 2 + 1, out[:dests, lanes:] - out[dests:, :lanes]


def y_pack_kernel(rows, keep_ref, got_ref, table_ref, _, out_ref):
    dests = table_ref.shape[2] // 2
    per = out_ref.shape[0] // dests
    for block, q, value in y_blocks(keep_ref, got_ref, table_ref, rows):
        out_ref[pl.ds(block * 4 + q, dests, per), :] = value


def y_send_kernel(rows, keep_ref, got_ref, table_ref, *refs):
    outs, all_ref = refs[:-1], refs[-1]
    dests = table_ref.shape[2] // 2
    for block, q, value in y_blocks(keep_ref, got_ref, table_ref, rows):
        at = (block * 4 + q) * dests
        all_ref[at : at + dests] = value
    _, z, _ = place()
    for shift in range(NZ):
        to = lax.rem(z - shift + NZ, NZ)
        for k in range(all_ref.shape[0] // dests):
            outs[shift][k * NXY : (k + 1) * NXY] = all_ref[pl.ds(pl.multiple_of(k * dests + to * NXY, NXY), NXY), :]


def turn_kernel(*refs):
    gots, outs, all_ref = refs[:NZ], refs[NZ:-1], refs[-1]
    y, z, x = place()
    size = gots[0].shape[0]
    for shift in range(NZ):
        source = lax.rem(z + shift, NZ)
        all_ref[pl.ds(pl.multiple_of(source * size, size), size), :] = gots[shift][...]
    count = all_ref.shape[0] // NXY
    for dy in range(NY):
        for dx in range(NX):
            to = lax.rem(y - dy + NY, NY) * NX + lax.rem(x - dx + NX, NX)
            outs[dy * NX + dx][...] = all_ref[pl.ds(to, count, NXY), :]


def wave_numbers(keep, lanes, first, count, step):
    group = lax.axis_index("section") * lax.axis_size("pen") + lax.axis_index("pen")
    limit = -(keep // 2)
    visc = 0.5 / (keep // 2) ** 2
    row = lax.broadcasted_iota(jnp.int32, (count, lanes), 0) * step + first
    col = lax.broadcasted_iota(jnp.int32, (count, lanes), 1) + lax.axis_index("slab") * lanes
    kz = jnp.where(row < keep // 2, row, row - keep)
    kx = jnp.where(col < keep // 2, col, col - keep)
    for parity in range(2):
        index = group * 2 + parity
        ky = jnp.where(index < keep // 2, index, index - keep)
        mask = ((kx != limit) & (kz != limit) & (ky != limit)).astype(jnp.float32)
        waves = (kx.astype(jnp.float32), ky.astype(jnp.float32), kz.astype(jnp.float32))
        ksq = waves[0] * waves[0] + waves[1] * waves[1] + waves[2] * waves[2]
        yield parity, waves, mask, 1.0 / jnp.maximum(ksq, 1.0), visc * ksq


def projected(s, waves, mask, inverse):
    inner = (waves[0] * s[0] + waves[1] * s[1] + waves[2] * s[2]) * inverse
    return [mask * (s[c] - waves[c] * inner) for c in range(3)]


def z_sums(keep, lanes, table, columns):
    out = transformed(table[0], table[1], columns)
    return out[:keep, :lanes] + out[keep:, lanes:], out[:keep, lanes:] - out[keep:, :lanes]


def early_kernel(keep, *refs):
    gots, (modes_hbm, table_ref, out_ref, all_ref, modes_ref, sems) = refs[:NXY], refs[NXY:]
    copies = []
    part = modes_ref.shape[0] // sems.shape[0]
    for i in range(sems.shape[0]):
        rows = pl.ds(i * part, part)
        copies.append(pltpu.make_async_copy(modes_hbm.at[rows], modes_ref.at[rows], sems.at[i]))
        copies[-1].start()
    y, _, x = place()
    lanes = out_ref.shape[1]
    kinds = gots[0].shape[0] // NZ
    sources = NXY * NZ
    for dy in range(NY):
        for dx in range(NX):
            source = lax.rem(y + dy, NY) * NX + lax.rem(x + dx, NX)
            for k in range(kinds):
                at = pl.multiple_of(k * sources + source * NZ, NZ)
                all_ref[pl.ds(at, NZ), :] = gots[dy * NX + dx][pl.ds(k, NZ, kinds), :]
    sums = []
    for parity in range(2):
        for c in range(3):
            base = c * 4 + parity * 2
            both = [all_ref[(base + q) * sources : (base + q + 1) * sources] for q in range(2)]
            sums.append(z_sums(keep, lanes, table_ref, jnp.concatenate(both, axis=1)))
    for copy in copies:
        copy.wait()
    for parity, waves, mask, inverse, damp in wave_numbers(keep, lanes, 0, keep, 1):
        for q in range(2):
            s = [sums[parity * 3 + c][q] for c in range(3)]
            for c, value in enumerate(projected(s, waves, mask, inverse)):
                where = pl.ds(c * keep * 4 + parity * 2 + q, keep, 4)
                at = ((c * 2 + parity) * 2 + q) * keep
                out_ref[at : at + keep] = value - damp * modes_ref[where, :]


def z_kernel(planes, keep, x_ref, early_ref, table_ref, out_hbm, sums_ref, out_ref, sems):
    lanes = x_ref.shape[1]
    per = 3 * planes * 4
    sources = x_ref.shape[0] // per
    run = NXY // 2
    for parity in range(2):
        for c in range(3):
            sums, differences = [], []
            for p in range(planes):
                at = (p * 3 + c) * 4 + parity * 2
                both = jnp.concatenate([x_ref[pl.ds(at + q, sources, per), :] for q in range(2)], axis=1)
                both = both.reshape(NZ, 2, run, 2 * lanes)
                sums.append((both[:, 0] + both[:, 1]).reshape(NZ * run, 2 * lanes))
                differences.append((both[:, 0] - both[:, 1]).reshape(NZ * run, 2 * lanes))
            for e, folded in enumerate((sums, differences)):
                pair = z_sums(keep // 2, lanes, table_ref.at[e], jnp.concatenate(folded, axis=0))
                for q in range(2):
                    sums_ref[parity, q, c, e] = pair[q]
    count = sems.shape[0] // 3
    part = keep // 2 // count
    copies = []
    for h in range(count):
        here = slice(h * part, (h + 1) * part)
        for e in range(2):
            for parity, waves, mask, inverse, _ in wave_numbers(keep, lanes, h * part * 2 + e, part, 2):
                for q in range(2):
                    values = projected([sums_ref[parity, q, c, e, here] for c in range(3)], waves, mask, inverse)
                    for c, value in enumerate(values):
                        where = pl.ds((c * keep + h * part * 2 + e) * 4 + parity * 2 + q, part, 8)
                        at = ((c * 2 + parity) * 2 + q) * keep + h * part * 2 + e
                        out_ref[where, :] = value + early_ref[pl.ds(at, part, 2), :]
        for c in range(3):
            rows = pl.ds((c * keep + h * part * 2) * 4, part * 8)
            copies.append(pltpu.make_async_copy(out_ref.at[rows], out_hbm.at[rows], sems.at[h * 3 + c]))
            copies[-1].start()
    for copy in copies:
        copy.wait()


def call(kernel, outs, flops=0, scratch=(), space=VMEM, out_space=VMEM, limit=40 << 20, kind=jnp.float32):
    def run(*args):
        size = sum(a.size * a.dtype.itemsize for a in args) + sum(4 * math.prod(o) for o in outs)
        shapes = [jax.ShapeDtypeStruct(o, kind) for o in outs]
        specs = [pl.BlockSpec(memory_space=out_space)] * len(outs)
        single = len(outs) == 1
        return pl.pallas_call(
            kernel,
            out_shape=shapes[0] if single else shapes,
            in_specs=[pl.BlockSpec(memory_space=m) for m in (space if isinstance(space, list) else [space] * len(args))],
            out_specs=specs[0] if single else specs,
            scratch_shapes=list(scratch),
            cost_estimate=pl.CostEstimate(flops=flops, bytes_accessed=size, transcendentals=0),
            compiler_params=pltpu.CompilerParams(vmem_limit_bytes=limit),
        )(*args)

    return run


def group_of(y, z, x):
    return ((y % NY) * NZ + z % NZ) * NX + x % NX


def from_shift(value, dy, dz, dx):
    pairs = [
        (group_of(y + dy, z + dz, x + dx), group_of(y, z, x))
        for y in range(NY)
        for z in range(NZ)
        for x in range(NX)
    ]
    return lax.ppermute(value, GROUP, pairs)


def per_device(velocity, vorticity, velocity_modes):
    _, planes, rows_y, cells = velocity.shape
    _, keep, rows_ky, _, lanes = velocity_modes.shape
    dests = lax.axis_size(GROUP)
    order = z_major_groups()
    table_y = jnp.asarray(y_table(cells, keep, order))
    table_x = jnp.asarray(x_table(cells, keep))
    crosses = call(
        cross_kernel,
        [(3 * rows_y, 2 * cells)] * planes,
        6 * planes * 3 * rows_y * cells,
        [VMEM((planes, 3, rows_y, cells), jnp.float32)] * 2 + [pltpu.SemaphoreType.DMA((12 * planes,))],
        pltpu.HBM,
        limit=50 << 20,
        kind=jnp.bfloat16,
    )(velocity, vorticity)
    keeps, gots = [], []
    for held in (crosses[:1], crosses[1:]):
        n = len(held)
        run = call(x_kernel, [(3 * n * rows_y, keep)] * 2, 2 * 9 * n * rows_y * cells * 2 * keep)
        mine, other = run(*held, table_x)
        keeps.append(mine)
        gots.append(lax.ppermute(other, "slab", [(0, 1), (1, 0)]))
    flops = 2 * 3 * 2 * keep * 3 * rows_y * keep
    kinds = 3 * 4
    sent = call(
        functools.partial(y_send_kernel, rows_y),
        [(kinds * NXY, lanes)] * NZ,
        flops,
        [VMEM((kinds * dests, lanes), jnp.float32)],
    )(keeps[0], gots[0], table_y)
    arrived = [sent[0]]
    for s in range(1, NZ):
        arrived.append(from_shift(sent[s], 0, s, 0))
    per = (planes - 1) * kinds
    packed = call(
        functools.partial(y_pack_kernel, rows_y), [(dests * per, lanes)], flops * (planes - 1)
    )(keeps[1], gots[1], table_y, sent[0])
    late = lax.all_to_all(
        packed.reshape(dests, per, lanes), GROUP, 0, 0, axis_index_groups=[order.tolist()], tiled=True
    )
    turned = call(turn_kernel, [(NZ * kinds, lanes)] * NXY, 0, [VMEM((NZ * kinds * NXY, lanes), jnp.float32)])(*arrived)
    spread = [turned[0]] + [from_shift(turned[d], d // NX, 0, d % NX) for d in range(1, NXY)]
    early = call(
        functools.partial(early_kernel, keep),
        [(3 * keep * 4, lanes)],
        2 * 6 * 2 * keep * 3 * dests * keep,
        [
            VMEM((kinds * dests, lanes), jnp.float32),
            VMEM((3 * keep * 4, lanes), jnp.float32),
            pltpu.SemaphoreType.DMA((12,)),
        ],
        [VMEM] * NXY + [pltpu.HBM, VMEM],
        limit=50 << 20,
    )(
        *spread,
        velocity_modes.reshape(3 * keep * 4, lanes),
        jnp.asarray(z_table(cells, keep, planes * xy_major_groups())),
    )
    near = order.reshape(NZ, 2, -1)[:, 0].reshape(-1)
    rest = np.concatenate([planes * near + p for p in range(1, planes)])
    table_z = jnp.asarray(folded_z_table(cells, keep, rest))
    out = call(
        functools.partial(z_kernel, planes - 1, keep),
        [(3 * keep * 4, lanes)],
        6 * 2 * keep * 3 * (planes - 1) * dests * keep,
        [
            VMEM((2, 2, 3, 2, keep // 2, lanes), jnp.float32),
            VMEM((3 * keep * 4, lanes), jnp.float32),
            pltpu.SemaphoreType.DMA((6,)),
        ],
        out_space=pltpu.HBM,
    )(late.reshape(dests * per, lanes), early, table_z)
    return out.reshape(3, keep, rows_ky, 2, lanes)


def solution(mesh):
    return jax.shard_map(
        per_device,
        mesh=mesh,
        in_specs=(
            P(None, GROUP, "slab", None),
            P(None, GROUP, "slab", None),
            P(None, None, GROUP, None, "slab"),
        ),
        out_specs=P(None, None, GROUP, None, "slab"),
        check_vma=False,
    )
```
